32 devices in a mesh: dp: 32 (over z, y, x, core).
Axes of the slice: x: 2, y: 2, z: 4, core: 2. Of those that a mesh axis runs over, the one named last changes fastest.
Arguments:
- hidden: bfloat16 [24576, 2560], P('dp'), may hold values from -16 to 16
- rotation: bfloat16 [2560, 2560], P('dp'), may hold values from -1 to 1, as said below
- norm_gain: float32 [2, 2560], replicated, may hold values from 0.1 to 1.9
- value_weight: bfloat16 [2, 2560, 1024], P(None, None, 'dp'), may hold values from -0.125 to 0.125
- output_weight: bfloat16 [2, 1024, 2560], P(None, 'dp'), may hold values from -0.1875 to 0.1875
- lengths: int32 [32], replicated, may hold values from 1 to 768, as said below
Outputs:
- rotated_out: bfloat16 [24576, 2560], P('dp')
- calib_loss: float32 [], replicated
The draws below stay inside these ranges and needn't reach their ends.
Inputs may be any that keep to these rules, and one draw needn't show every extreme that they name: `lengths`: some device has all of its 768 rows live. `rotation`: an orthogonal matrix rounded to bfloat16.
All inputs are finite; a program needn't handle non-finite values.
Results may differ from the reference program's by a relative error of at most 0.0088.
Values may be sent and summed in bfloat16 or wider, within the bound.
A program may use at most 192 MiB of HBM per device.

```python
import jax
import jax.numpy as jnp
from jax import lax

D = 2560
E = 1024
BLOCK = 256
SLOTS = 3
LAYERS = 2
ROWS_DEV = 768
ROWS = 24576
N_DP = 32


def draw_hidden(key, part):
    noise_key, factor_key = jax.random.split(key)
    samples = jax.random.normal(noise_key, (ROWS, D), jnp.float32)
    row_factor = jnp.exp(jax.random.uniform(factor_key, (ROWS, 1), jnp.float32, -0.35, 0.35))
    rising = 0.5 + jnp.arange(ROWS, dtype=jnp.float32)[:, None] / ROWS
    return jnp.clip(samples * rising * row_factor, -16.0, 16.0).astype(jnp.bfloat16)


def draw_rotation(key, part):
    samples = jax.random.normal(key, (D, D), jnp.float32)
    orthogonal, triangle = jnp.linalg.qr(samples)
    return orthogonal.astype(jnp.bfloat16)


def draw_lengths(key, part):
    full_span = SLOTS * BLOCK
    draw_key, pick_key = jax.random.split(key)
    uniform_ints = jax.random.randint(draw_key, (N_DP,), 0, full_span)
    skewed = 1 + uniform_ints * uniform_ints // full_span
    chosen = jax.random.randint(pick_key, (), 0, N_DP)
    return jnp.where(jnp.arange(N_DP) == chosen, full_span, skewed).astype(jnp.int32)


def block_levels(key, dims, cuts, smallest, top_value):
    factor_of = 1.0
    for dim, blocks in cuts:
        draws = jax.random.uniform(jax.random.fold_in(jax.random.fold_in(key, 6), dim), (blocks,), jnp.float32, smallest / len(cuts), top_value / len(cuts))
        factor_of = factor_of * jnp.repeat(jnp.exp(draws), dims[dim] // blocks).reshape((-1,) + (1,) * (len(dims) - 1 - dim))
    return factor_of


def bell_draw(own_key, extent, deviation, bound, cuts=(), kind=jnp.bfloat16):
    loudness = block_levels(own_key, extent, cuts, -0.22, 0.18) if cuts else 1.0
    drawn = jax.random.normal(own_key, extent, jnp.float32) * deviation * loudness
    return jnp.minimum(jnp.maximum(drawn, -bound), bound).astype(kind)


def setup_inputs(seed: int = 0) -> dict:
    key_list = jax.random.split(jax.random.key(seed), 7)
    return {
        "hidden": draw_hidden(jax.random.fold_in(key_list[6], 71), 0),
        "rotation": draw_rotation(jax.random.fold_in(key_list[6], 71), 0),
        "norm_gain": jnp.clip(1.0 + 0.18 * jax.random.normal(key_list[2], (LAYERS, D), jnp.float32), 0.1, 1.9),
        "value_weight": bell_draw(key_list[3], (LAYERS, D, E), D ** -0.5, 0.125, ((2, 32),)),
        "output_weight": bell_draw(key_list[4], (LAYERS, E, D), E ** -0.5, 0.1875, ((1, 32),)),
        "lengths": draw_lengths(jax.random.fold_in(key_list[6], 71), 0),
    }


EPS_NORM = 1e-06
EPS_SCALE = 1e-06
CLIP_RATIO = 0.9
TWO_PI = 6.283185307179586

def soft_round(values):
    return values - jnp.sin(TWO_PI * values) / TWO_PI

def fake_quant(values, step_size):
    return soft_round(jnp.clip(values / step_size, -8.0, 7.0)) * step_size

def quant_columns(matrix):
    step_size = lax.optimization_barrier(jnp.max(jnp.abs(matrix), axis=0)) / 7.0 + EPS_SCALE
    return fake_quant(matrix, step_size[None, :]).astype(jnp.bfloat16)

def reference(hidden, rotation, norm_gain, value_weight, output_weight, lengths):
    positions = lax.broadcasted_iota(jnp.int32, (N_DP, ROWS_DEV), 1)
    live_rows = positions < lengths[:, None]
    count = jnp.sum(lengths).astype(jnp.float32)
    blocks = hidden.reshape(N_DP, ROWS_DEV, D)
    resid = lax.map(lambda block_rows: jnp.dot(block_rows.astype(jnp.float32), rotation.astype(jnp.float32), preferred_element_type=jnp.float32), blocks)
    loss_sum = jnp.zeros((), jnp.float32)
    for layer_number in range(LAYERS):
        scaled = (norm_gain[layer_number][:, None] * value_weight[layer_number].astype(jnp.float32)).astype(jnp.bfloat16)
        rotated_v = lax.dot_general(rotation.astype(jnp.float32), scaled.astype(jnp.float32), (((0,), (0,)), ((), ())), preferred_element_type=jnp.float32)
        value_q = quant_columns(rotated_v)
        rotated_o = jnp.dot(output_weight[layer_number].astype(jnp.float32), rotation.astype(jnp.float32), preferred_element_type=jnp.float32)
        output_q = quant_columns(rotated_o)

        def first_pass(operands):
            residual, live_mask = operands
            mean_sq = lax.optimization_barrier(jnp.mean(residual * residual, axis=1))
            normed = residual * lax.rsqrt(mean_sq + EPS_NORM)[:, None]
            step_size = CLIP_RATIO * lax.optimization_barrier(jnp.max(jnp.abs(normed), axis=1)) / 7.0 + EPS_SCALE
            act_f = fake_quant(normed, step_size[:, None])
            act_err = lax.optimization_barrier(jnp.sum((act_f - normed) * (act_f - normed), axis=1))
            mixed = jnp.dot(act_f.astype(jnp.bfloat16).astype(jnp.float32), value_q.astype(jnp.float32), preferred_element_type=jnp.float32)
            channel_top = lax.optimization_barrier(jnp.max(jnp.where(live_mask[:, None], jnp.abs(mixed), 0.0), axis=0))
            return (mean_sq, act_err, mixed, channel_top)
        mean_sq, act_err, mixed, channel_top = lax.map(first_pass, (resid, live_rows))
        vrange = lax.optimization_barrier(jnp.max(channel_top, axis=0))
        mix_step = CLIP_RATIO * vrange / 7.0 + EPS_SCALE

        def second_pass(operands):
            residual, mixed_rows = operands
            mix_f = fake_quant(mixed_rows, mix_step[None, :])
            mix_err = lax.optimization_barrier(jnp.sum((mix_f - mixed_rows) * (mix_f - mixed_rows), axis=1))
            updated = residual + jnp.dot(mix_f.astype(jnp.bfloat16).astype(jnp.float32), output_q.astype(jnp.float32), preferred_element_type=jnp.float32)
            return (updated, mix_err)
        resid, mix_err = lax.map(second_pass, (resid, mixed))
        loss_sum = loss_sum + jnp.sum(jnp.where(live_rows, mean_sq * (act_err + mix_err), 0.0))
    rotated_out = jnp.where(live_rows[:, :, None], resid, 0.0).astype(jnp.bfloat16).reshape(ROWS, D)
    return (rotated_out, loss_sum / count)
```

```python
import functools

import jax
import jax.numpy as jnp
from jax import lax
from jax.experimental import pallas as pl
from jax.experimental.pallas import tpu as pltpu
from jax.sharding import PartitionSpec as P

BLOCK = 256
CHUNK = 16
TILE = 512
VMEM_LIMIT = 60 * 1024 * 1024

EPS_NORM = 1e-06
EPS_SCALE = 1e-06
CLIP_RATIO = 0.9
POLY = (0.9999997571452157, -2.579687436847881, 2.6673586060553345, -1.5145036626283546, 0.48039577352173)


def soft_round(values):
    r = values - jnp.round(values)
    u = r * r
    p = jnp.float32(POLY[-1])
    for c in POLY[-2::-1]:
        p = p * u + jnp.float32(c)
    return values - p * (r - 4.0 * (r * u))


def fake_quant(values, step_size):
    inv = 1.0 / step_size
    return soft_round(jnp.clip(values * inv, -8.0, 7.0)) * step_size


def exchange_kernel(n, total, x_ref, out_ref, slots, send_sem, recv_sem):
    me = lax.axis_index("dp")
    barrier = pltpu.get_barrier_semaphore()

    def greet(k, _):
        pl.semaphore_signal(
            barrier,
            inc=1,
            device_id=(lax.rem(me + k, n),),
            device_id_type=pl.DeviceIdType.MESH,
        )
        return 0

    lax.fori_loop(1, n, greet, 0)
    pl.semaphore_wait(barrier, n - 1)

    def copy_to(peer, slot):
        return pltpu.make_async_remote_copy(
            src_ref=x_ref,
            dst_ref=slots.at[slot],
            send_sem=send_sem.at[peer],
            recv_sem=recv_sem.at[slot],
            device_id=(peer,),
            device_id_type=pl.DeviceIdType.MESH,
        )

    def push(k, _):
        copy_to(lax.rem(me + k, n), me).start()
        return 0

    lax.fori_loop(1, n, push, 0)
    slots[me] = x_ref[...]

    def settle(k, _):
        peer = lax.rem(me + k, n)
        copy = copy_to(peer, peer)
        copy.wait_send()
        copy.wait_recv()
        return 0

    lax.fori_loop(1, n, settle, 0)

    def fold(k, acc):
        return acc + slots[k] if total else jnp.maximum(acc, slots[k])

    out_ref[...] = lax.fori_loop(1, n, fold, slots[0])


def exchange(x, n, collective_id, total=False):
    return pl.pallas_call(
        functools.partial(exchange_kernel, n, total),
        name="exchange",
        in_specs=[pl.BlockSpec(memory_space=pltpu.VMEM)],
        out_specs=pl.BlockSpec(memory_space=pltpu.VMEM),
        out_shape=jax.ShapeDtypeStruct(x.shape, x.dtype),
        scratch_shapes=[
            pltpu.VMEM((n,) + x.shape, x.dtype),
            pltpu.SemaphoreType.DMA((n,)),
            pltpu.SemaphoreType.DMA((n,)),
        ],
        compiler_params=pltpu.CompilerParams(
            collective_id=collective_id, has_side_effects=True, vmem_limit_bytes=VMEM_LIMIT
        ),
        cost_estimate=pl.CostEstimate(flops=0, bytes_accessed=30_000_000, transcendentals=0),
    )(x)


def weight_kernel(v_rows, o_rows, layers, w_ref, r_ref, vq_ref, o_ref, top_ref, acc):
    j = pl.program_id(0)
    n = r_ref.shape[1]
    at = pl.ds(pl.multiple_of(j * n, n), n)
    prod = jnp.dot(w_ref[...], r_ref[...], preferred_element_type=jnp.float32)
    acc[:, at] = prod[:v_rows]
    o_ref[...] = prod[v_rows:]
    per = o_rows // layers
    for l in range(layers):
        lo = v_rows + l * per
        top_ref[l : l + 1, :] = jnp.max(jnp.abs(prod[lo : lo + per]), axis=0, keepdims=True)

    @pl.when(j == pl.num_programs(0) - 1)
    def _():
        def body(i, _):
            rows = pl.ds(pl.multiple_of(i * CHUNK, CHUNK), CHUNK)
            x = acc[rows, :]
            step = jnp.max(jnp.abs(x), axis=1, keepdims=True) / 7.0 + EPS_SCALE
            vq_ref[rows, :] = fake_quant(x, step).astype(jnp.bfloat16)
            return 0

        lax.fori_loop(0, v_rows // CHUNK, body, 0)


def rotate_weights(joined, rotation, v_rows, o_rows, layers):
    width = rotation.shape[1]
    depth = rotation.shape[0]
    return pl.pallas_call(
        functools.partial(weight_kernel, v_rows, o_rows, layers),
        name="rotate_weights",
        grid=(width // TILE,),
        in_specs=[
            pl.BlockSpec(joined.shape, lambda j: (0, 0)),
            pl.BlockSpec((depth, TILE), lambda j: (0, j)),
        ],
        out_specs=[
            pl.BlockSpec((v_rows, width), lambda j: (0, 0)),
            pl.BlockSpec((o_rows, TILE), lambda j: (0, j)),
            pl.BlockSpec((layers, TILE), lambda j: (0, j)),
        ],
        out_shape=[
            jax.ShapeDtypeStruct((v_rows, width), jnp.bfloat16),
            jax.ShapeDtypeStruct((o_rows, width), jnp.float32),
            jax.ShapeDtypeStruct((layers, width), jnp.float32),
        ],
        scratch_shapes=[pltpu.VMEM((v_rows, width), jnp.float32)],
        compiler_params=pltpu.CompilerParams(vmem_limit_bytes=VMEM_LIMIT),
        cost_estimate=pl.CostEstimate(
            flops=2 * joined.shape[0] * depth * width,
            bytes_accessed=2 * depth * width,
            transcendentals=0,
        ),
    )(joined, rotation)


def norm_rows(resid_ref, act_ref, msq_ref, aerr_ref):
    width = resid_ref.shape[1]

    def body(i, _):
        rows = pl.ds(pl.multiple_of(i * CHUNK, CHUNK), CHUNK)
        x = resid_ref[rows, :]
        mean_sq = jnp.sum(x * x, axis=1, keepdims=True) * (1.0 / width)
        inv = lax.rsqrt(mean_sq + EPS_NORM)
        step = CLIP_RATIO * (jnp.max(jnp.abs(x), axis=1, keepdims=True) * inv) / 7.0 + EPS_SCALE
        normed = x * inv
        act = fake_quant(normed, step)
        diff = act - normed
        act_ref[rows, :] = act.astype(jnp.bfloat16)
        msq_ref[rows, :] = mean_sq
        aerr_ref[rows, :] = jnp.sum(diff * diff, axis=1, keepdims=True)
        return 0

    lax.fori_loop(0, resid_ref.shape[0] // CHUNK, body, 0)


def first_kernel(h_ref, r_ref, resid_ref, act_ref, msq_ref, aerr_ref):
    def body(j, _):
        at = pl.ds(pl.multiple_of(j * TILE, TILE), TILE)
        resid_ref[:, at] = jnp.dot(h_ref[...], r_ref[:, at], preferred_element_type=jnp.float32)
        return 0

    lax.fori_loop(0, r_ref.shape[1] // TILE, body, 0)
    norm_rows(resid_ref, act_ref, msq_ref, aerr_ref)


def rows_spec(width):
    return pl.BlockSpec((BLOCK, width), lambda i, *_: (i, 0))


def whole_spec(shape):
    return pl.BlockSpec(shape, lambda i, *_: (0, 0), pipeline_mode=pl.Buffered(1))


def act_shapes(rows, width):
    return [
        jax.ShapeDtypeStruct((rows, width), jnp.float32),
        jax.ShapeDtypeStruct((rows, width), jnp.bfloat16),
        jax.ShapeDtypeStruct((rows, 1), jnp.float32),
        jax.ShapeDtypeStruct((rows, 1), jnp.float32),
    ]


def first_pass(hidden, rotation):
    rows, depth = hidden.shape
    width = rotation.shape[1]
    return pl.pallas_call(
        first_kernel,
        name="rotate_hidden",
        grid=(rows // BLOCK,),
        in_specs=[rows_spec(depth), whole_spec(rotation.shape)],
        out_specs=[rows_spec(width), rows_spec(width), rows_spec(1), rows_spec(1)],
        out_shape=act_shapes(rows, width),
        compiler_params=pltpu.CompilerParams(vmem_limit_bytes=VMEM_LIMIT),
        cost_estimate=pl.CostEstimate(
            flops=2 * rows * depth * width,
            bytes_accessed=2 * depth * width + 8 * rows * width,
            transcendentals=0,
        ),
    )(hidden, rotation)


def mix_kernel(len_ref, act_ref, v_ref, mixed_ref, top_ref):
    i = pl.program_id(0)
    tile = 256
    live = len_ref[0] - i * BLOCK
    mask = lax.broadcasted_iota(jnp.int32, (BLOCK, 1), 0) < live

    @pl.when(i == 0)
    def _():
        top_ref[...] = jnp.zeros_like(top_ref)

    cols = v_ref.shape[1]
    group = tile // cols

    def body(j, _):
        at = pl.ds(pl.multiple_of(j * tile, tile), tile)
        part = v_ref[pl.ds(j * group, group)]
        prod = lax.dot_general(
            act_ref[...],
            part.reshape(tile, part.shape[2]),
            (((1,), (1,)), ((), ())),
            preferred_element_type=jnp.float32,
        )
        mixed_ref[:, at] = prod
        peak = jnp.max(jnp.where(mask, jnp.abs(prod), 0.0), axis=0, keepdims=True)
        top_ref[:, at] = jnp.maximum(top_ref[:, at], peak)
        return 0

    lax.fori_loop(0, v_ref.shape[0] // group, body, 0)


def mix_pass(own_len, act, gathered, layer, cols):
    rows, width = act.shape
    n = gathered.shape[0]
    channels = n * cols
    if cols % 16 == 0:
        values = gathered
        spec = pl.BlockSpec(
            (n, cols, width), lambda i, *_: (0, layer, 0), pipeline_mode=pl.Buffered(1)
        )
    else:
        values = gathered[:, layer * cols : (layer + 1) * cols].reshape(-1, 128, width)
        spec = pl.BlockSpec(values.shape, lambda i, *_: (0, 0, 0), pipeline_mode=pl.Buffered(1))
    return pl.pallas_call(
        mix_kernel,
        name="mix",
        grid_spec=pltpu.PrefetchScalarGridSpec(
            num_scalar_prefetch=1,
            grid=(rows // BLOCK,),
            in_specs=[rows_spec(width), spec],
            out_specs=[
                rows_spec(channels),
                pl.BlockSpec((1, channels), lambda i, *_: (0, 0)),
            ],
        ),
        out_shape=[
            jax.ShapeDtypeStruct((rows, channels), jnp.float32),
            jax.ShapeDtypeStruct((1, channels), jnp.float32),
        ],
        compiler_params=pltpu.CompilerParams(vmem_limit_bytes=VMEM_LIMIT),
        cost_estimate=pl.CostEstimate(
            flops=2 * rows * channels * width,
            bytes_accessed=2 * channels * width + 4 * rows * width,
            transcendentals=0,
        ),
    )(own_len, act, values)


def update_kernel(last, len_ref, mixed_ref, vrange_ref, o_ref, resid_ref, msq_ref, aerr_ref, *rest):
    if last:
        loss_ref, out_ref, mix_buf = rest
    else:
        loss_ref, new_ref, act_ref, nmsq_ref, naerr_ref, mix_buf = rest
    live = len_ref[0] - pl.program_id(0) * BLOCK
    mask = lax.broadcasted_iota(jnp.int32, (BLOCK, 1), 0) < live
    step = CLIP_RATIO * vrange_ref[...] / 7.0 + EPS_SCALE

    def quant(i, _):
        rows = pl.ds(pl.multiple_of(i * CHUNK, CHUNK), CHUNK)
        x = mixed_ref[rows, :]
        mix = fake_quant(x, step)
        diff = mix - x
        mix_buf[rows, :] = mix.astype(jnp.bfloat16)
        loss_ref[rows, :] = jnp.sum(diff * diff, axis=1, keepdims=True)
        return 0

    lax.fori_loop(0, BLOCK // CHUNK, quant, 0)
    loss_ref[...] = jnp.where(mask, msq_ref[...] * (aerr_ref[...] + loss_ref[...]), 0.0)

    def body(j, _):
        at = pl.ds(pl.multiple_of(j * TILE, TILE), TILE)
        new = resid_ref[:, at] + jnp.dot(
            mix_buf[...], o_ref[:, at], preferred_element_type=jnp.float32
        )
        if last:
            out_ref[:, at] = jnp.where(mask, new, 0.0).astype(jnp.bfloat16)
        else:
            new_ref[:, at] = new
        return 0

    lax.fori_loop(0, o_ref.shape[1] // TILE, body, 0)
    if not last:
        norm_rows(new_ref, act_ref, nmsq_ref, naerr_ref)


def update_pass(own_len, mixed, vrange, outputs, resid, msq, aerr, last):
    rows, width = resid.shape
    channels = mixed.shape[1]
    out_specs = [rows_spec(1)]
    out_shape = [jax.ShapeDtypeStruct((rows, 1), jnp.float32)]
    if last:
        out_specs.append(rows_spec(width))
        out_shape.append(jax.ShapeDtypeStruct((rows, width), jnp.bfloat16))
    else:
        out_specs += [rows_spec(width), rows_spec(width), rows_spec(1), rows_spec(1)]
        out_shape += act_shapes(rows, width)
    return pl.pallas_call(
        functools.partial(update_kernel, last),
        name="update",
        grid_spec=pltpu.PrefetchScalarGridSpec(
            num_scalar_prefetch=1,
            grid=(rows // BLOCK,),
            in_specs=[
                rows_spec(channels),
                whole_spec((1, channels)),
                whole_spec(outputs.shape),
                rows_spec(width),
                rows_spec(1),
                rows_spec(1),
            ],
            out_specs=out_specs,
            scratch_shapes=[pltpu.VMEM((BLOCK, channels), jnp.bfloat16)],
        ),
        out_shape=out_shape,
        compiler_params=pltpu.CompilerParams(vmem_limit_bytes=VMEM_LIMIT),
        cost_estimate=pl.CostEstimate(
            flops=2 * rows * channels * width,
            bytes_accessed=2 * channels * width + 12 * rows * width,
            transcendentals=0,
        ),
    )(own_len, mixed, vrange, outputs, resid, msq, aerr)


MESH_ID = pl.DeviceIdType.MESH
FULL_VMEM = 67043328
PIECES = 3


class Place:
    def __init__(self, n):
        me = lax.axis_index("dp")
        core = lax.rem(me, 2)
        self.me, self.planes, self.core = me, n // 8, core
        self.z = me // 8
        self.stride2 = 2 + 2 * core
        self.stride3 = 4 - 2 * core
        self.bit2 = lax.rem(me // self.stride2, 2)
        self.bit3 = lax.rem(me // self.stride3, 2)
        self.to = [
            me + 8,
            me - 8,
            me + self.stride2 * (1 - 2 * self.bit2),
            me + self.stride3 * (1 - 2 * self.bit3),
            me + 1 - 2 * core,
        ]

    def origin(self, plane, flip2, flip3):
        bit2 = 1 - self.bit2 if flip2 else self.bit2
        bit3 = 1 - self.bit3 if flip3 else self.bit3
        return 8 * plane + self.core + self.stride2 * bit2 + self.stride3 * bit3

    def at_distance(self, s):
        if s == 0:
            return [(self.z, None)]
        return [(self.z - s, self.z >= s), (self.z + s, self.z + s < self.planes)]

    def on_planes(self, s, piece):
        if s == 0:
            piece(self.z)
            return

        def body(k, _):
            plane = self.z - s + 2 * s * k
            pl.when(jnp.logical_and(plane >= 0, plane < self.planes))(lambda: piece(plane))
            return 0

        lax.fori_loop(0, 2, body, 0)

    def greet(self):
        barrier = pltpu.get_barrier_semaphore()
        peers = [8 * self.z + lax.rem(self.me + k, 8) for k in range(1, 8)]
        peers += [lax.rem(self.me + 8 * k, 8 * self.planes) for k in range(1, self.planes)]
        for peer in peers:
            pl.semaphore_signal(barrier, inc=1, device_id=(peer,), device_id_type=MESH_ID)
        pl.semaphore_wait(barrier, len(peers))


def run_if(cond, fn):
    if cond is None:
        fn()
    else:
        pl.when(cond)(fn)


def start(copy):
    copy.start()


def sent(copy):
    copy.wait_send()


class Gather:
    def __init__(self, place, buf, send_sem, recv_sem):
        self.place, self.buf, self.send_sem, self.recv_sem = place, buf, send_sem, recv_sem

    def copy(self, o, d):
        return pltpu.make_async_remote_copy(
            src_ref=self.buf.at[o],
            dst_ref=self.buf.at[o],
            send_sem=self.send_sem.at[d, o // 2],
            recv_sem=self.recv_sem.at[o],
            device_id=(self.place.to[d],),
            device_id_type=MESH_ID,
        )

    def arrived(self, o):
        self.copy(o, 4).wait_recv()

    def up(self, o, act):
        pl.when(self.place.z < self.place.planes - 1)(lambda: act(self.copy(o, 0)))

    def down(self, o, act):
        pl.when(self.place.z > 0)(lambda: act(self.copy(o, 1)))

    def own(self, act=start):
        o = self.place.me
        self.up(o, act)
        self.down(o, act)
        for d in (2, 3, 4):
            act(self.copy(o, d))

    def line(self, s, act=start):
        for k, (plane, cond) in enumerate(self.place.at_distance(s)):

            def go(k=k, plane=plane):
                o = self.place.origin(plane, 0, 0)
                if act is start:
                    self.arrived(o)
                (self.up if k == 0 else self.down)(o, act)
                for d in (2, 3, 4):
                    act(self.copy(o, d))

            run_if(cond, go)

    def second(self, s, act=start):
        for plane, cond in self.place.at_distance(s):

            def go(plane=plane):
                o = self.place.origin(plane, 1, 0)
                if act is start:
                    self.arrived(o)
                for d in (3, 4):
                    act(self.copy(o, d))

            run_if(cond, go)

    def third(self, s, act=start):
        for plane, cond in self.place.at_distance(s):

            def go(plane=plane):
                for flip2 in (0, 1):
                    o = self.place.origin(plane, flip2, 1)
                    if act is start:
                        self.arrived(o)
                    act(self.copy(o, 4))

            run_if(cond, go)

    def other_core(self, s):
        for plane, cond in self.place.at_distance(s):

            def go(plane=plane):
                for q in range(4):
                    self.arrived(8 * plane + 2 * q + 1 - self.place.core)

            run_if(cond, go)

    def steps(self):
        return self.place.planes + 2

    def step(self, t):
        planes = self.place.planes
        if t == 0:
            self.own()
        elif t < planes:
            self.line(t)
        if 1 <= t < planes + 1:
            self.second(t - 1)
        if t >= 2:
            self.third(t - 2)
            self.other_core(t - 2)

    def drain(self):
        self.own(sent)
        for s in range(self.place.planes):
            if s:
                self.line(s, sent)
            self.second(s, sent)
            self.third(s, sent)


class Exchange:
    def __init__(self, place, total, near, far, near_send, near_recv, far_send, far_recv):
        self.place, self.total, self.near, self.far = place, total, near, far
        self.sems = (near_send, near_recv, far_send, far_recv)
        self.spot = lax.rem(place.me, 8)

    def near_copy(self, k, slot):
        spot = lax.rem(self.spot + k, 8)
        return pltpu.make_async_remote_copy(
            src_ref=self.near.at[slot],
            dst_ref=self.near.at[slot],
            send_sem=self.sems[0].at[k],
            recv_sem=self.sems[1].at[slot],
            device_id=(8 * self.place.z + spot,),
            device_id_type=MESH_ID,
        )

    def far_copy(self, k, slot):
        plane = lax.rem(self.place.z + k, self.place.planes)
        return pltpu.make_async_remote_copy(
            src_ref=self.far.at[slot],
            dst_ref=self.far.at[slot],
            send_sem=self.sems[2].at[k],
            recv_sem=self.sems[3].at[slot],
            device_id=(8 * plane + self.spot,),
            device_id_type=MESH_ID,
        )

    def fold(self, slots, count):
        acc = slots[0]
        for k in range(1, count):
            acc = acc + slots[k] if self.total else jnp.maximum(acc, slots[k])
        return acc

    def begin(self, value):
        self.near[self.spot] = value
        for k in range(1, 8):
            self.near_copy(k, self.spot).start()

    def middle(self):
        for k in range(1, 8):
            self.near_copy(k, lax.rem(self.spot + k, 8)).wait_recv()
        self.far[self.place.z] = self.fold(self.near, 8)
        for k in range(1, self.place.planes):
            self.far_copy(k, self.place.z).start()

    def end(self):
        for k in range(1, self.place.planes):
            self.far_copy(k, lax.rem(self.place.z + k, self.place.planes)).wait_recv()
        return self.fold(self.far, self.place.planes)

    def drain(self):
        for k in range(1, 8):
            self.near_copy(k, self.spot).wait_send()
        for k in range(1, self.place.planes):
            self.far_copy(k, self.place.z).wait_send()


def window_kernel(n, layers, *refs):
    len_ref, h_ref, w_ref, r_ref, out_ref, loss_ref = refs[:6]
    (rbuf, vbuf, obuf, resid, wacc, act, mixed, mixq, top, msq, aerr, lossrow) = refs[6:18]
    (ntops, ftops, ntop, ftop, nloss, floss) = refs[18:24]
    (local_sem, out_sem, rsend, rrecv, wsend, wrecv, xns, xnr, xfs, xfr) = refs[24:]
    place = Place(n)
    planes = place.planes
    rows, width = resid.shape
    cols = vbuf.shape[2]
    channels = n * cols
    depth = 8 * r_ref.shape[0]
    lanes = 8 * cols
    live = len_ref[place.me]

    mine = pltpu.make_async_copy(r_ref, rbuf.at[place.me], local_sem)
    mine.start()
    place.greet()
    mine.wait()

    rot = Gather(place, rbuf, rsend, rrecv)

    def rotate(first):
        def piece(plane):
            ks = pl.ds(pl.multiple_of(plane * depth, 128), depth)

            def body(j, _):
                at = pl.ds(pl.multiple_of(j * TILE, TILE), TILE)
                part = rbuf[pl.ds(8 * plane, 8), :, at].reshape(depth, TILE)
                a = jnp.dot(h_ref[:, ks], part, preferred_element_type=jnp.float32)
                w = jnp.dot(w_ref[:, ks], part, preferred_element_type=jnp.float32)
                if first:
                    resid[:, at] = a
                    wacc[:, at] = w
                else:
                    resid[:, at] += a
                    wacc[:, at] += w
                return 0

            lax.fori_loop(0, width // TILE, body, 0)

        return piece

    for t in range(rot.steps()):
        rot.step(t)
        if t >= 2:
            place.on_planes(t - 2, rotate(t == 2))

    vrows = layers * cols
    for l in range(layers):
        for i in range(cols // CHUNK):
            x = wacc[l * cols + i * CHUNK : l * cols + (i + 1) * CHUNK, :]
            step = jnp.max(jnp.abs(x), axis=1, keepdims=True) / 7.0 + EPS_SCALE
            vbuf[l, place.me, i * CHUNK : (i + 1) * CHUNK, :] = fake_quant(x, step).astype(jnp.bfloat16)

    gathers = []
    for l in range(layers):
        gathers.append(Gather(place, vbuf.at[l], wsend.at[2 * l], wrecv.at[2 * l]))
        gathers.append(Gather(place, obuf.at[l], wsend.at[2 * l + 1], wrecv.at[2 * l + 1]))

    def make(i, total, near, far):
        return Exchange(place, total, near, far, xns.at[i], xnr.at[i], xfs.at[i], xfr.at[i])

    tops = make(0, False, ntops, ftops)
    vranges = [make(1 + l, False, ntop.at[l], ftop.at[l]) for l in range(layers)]
    losses = make(1 + layers, True, nloss, floss)

    def norm(p):
        lo, hi = rows // CHUNK * p // PIECES, rows // CHUNK * (p + 1) // PIECES

        def body(i, _):
            at = pl.ds(pl.multiple_of(i * CHUNK, CHUNK), CHUNK)
            x = resid[at, :]
            mean_sq = jnp.sum(x * x, axis=1, keepdims=True) * (1.0 / width)
            inv = lax.rsqrt(mean_sq + EPS_NORM)
            step = CLIP_RATIO * (jnp.max(jnp.abs(x), axis=1, keepdims=True) * inv) / 7.0 + EPS_SCALE
            normed = x * inv
            q = fake_quant(normed, step)
            diff = q - normed
            act[at, :] = q.astype(jnp.bfloat16)
            msq[at, :] = mean_sq
            aerr[at, :] = jnp.sum(diff * diff, axis=1, keepdims=True)
            return 0

        lax.fori_loop(lo, hi, body, 0)

    def mix(l):
        def piece(plane):
            at = pl.ds(pl.multiple_of(plane * lanes, 128), lanes)
            part = vbuf[l, pl.ds(8 * plane, 8)].reshape(lanes, width)
            peak = jnp.zeros((1, lanes), jnp.float32)
            for b in range(rows // BLOCK):
                rs = slice(b * BLOCK, (b + 1) * BLOCK)
                prod = lax.dot_general(
                    act[rs, :], part, (((1,), (1,)), ((), ())), preferred_element_type=jnp.float32
                )
                mixed[rs, at] = prod
                mask = lax.broadcasted_iota(jnp.int32, (BLOCK, 1), 0) < live - b * BLOCK
                peak = jnp.maximum(
                    peak, jnp.max(jnp.where(mask, jnp.abs(prod), 0.0), axis=0, keepdims=True)
                )
            top[:, at] = peak

        return piece

    def quantize_mixed(l, vrange):
        step = CLIP_RATIO * vrange / 7.0 + EPS_SCALE

        def body(i, _):
            at = pl.ds(pl.multiple_of(i * CHUNK, CHUNK), CHUNK)
            x = mixed[at, :]
            q = fake_quant(x, step)
            diff = q - x
            mixq[at, :] = q.astype(jnp.bfloat16)
            mask = lax.broadcasted_iota(jnp.int32, (CHUNK, 1), 0) < live - i * CHUNK
            err = jnp.sum(diff * diff, axis=1, keepdims=True)
            row = jnp.where(mask, msq[at, :] * (aerr[at, :] + err), 0.0)
            if l == 0:
                lossrow[at, :] = row
            else:
                lossrow[at, :] += row
            return 0

        lax.fori_loop(0, rows // CHUNK, body, 0)

    def update(l):
        def piece(plane):
            ks = pl.ds(pl.multiple_of(plane * lanes, 128), lanes)

            def body(j, _):
                at = pl.ds(pl.multiple_of(j * TILE, TILE), TILE)
                part = obuf[l, pl.ds(8 * plane, 8), :, at].reshape(lanes, TILE)
                resid[:, at] += jnp.dot(mixq[:, ks], part, preferred_element_type=jnp.float32)
                return 0

            lax.fori_loop(0, width // TILE, body, 0)

        return piece

    normed, quantized = [0] * layers, [False] * layers
    waiting = [[] for _ in gathers]
    for k in range(planes * len(gathers) + 2):
        for g, gather in enumerate(gathers):
            t = k - planes * g
            if 0 <= t < gather.steps():
                gather.step(t)
                if t >= 2:
                    waiting[g].append(t - 2)
        if k == 0:
            tops.begin(
                jnp.concatenate(
                    [
                        jnp.max(
                            jnp.abs(wacc[vrows + l * cols : vrows + (l + 1) * cols, :]),
                            axis=0,
                            keepdims=True,
                        )
                        for l in range(layers)
                    ],
                    axis=0,
                )
            )
        if k == 1:
            tops.middle()
        if k == 2:
            peaks = tops.end()
            for l in range(layers):
                lo = vrows + l * cols
                obuf[l, place.me] = fake_quant(
                    wacc[lo : lo + cols, :], peaks[l : l + 1] / 7.0 + EPS_SCALE
                ).astype(jnp.bfloat16)
        for l in range(layers):
            t = k - 2 * planes * l
            ready = l == 0 or (quantized[l - 1] and t >= 1)
            if ready and normed[l] < PIECES and t >= 0:
                norm(normed[l])
                normed[l] += 1
            if normed[l] == PIECES:
                for s in waiting[2 * l]:
                    place.on_planes(s, mix(l))
                waiting[2 * l] = []
            if t == planes + 1:
                vranges[l].begin(top[...])
            if t == planes + 2:
                vranges[l].middle()
            if t == planes + 3:
                quantize_mixed(l, vranges[l].end())
                quantized[l] = True
                if l == layers - 1:
                    losses.begin(
                        jnp.broadcast_to(jnp.sum(lossrow[...], axis=0, keepdims=True), (1, 128))
                    )
            if t == planes + 4 and l == layers - 1:
                losses.middle()
            if quantized[l]:
                for s in waiting[2 * l + 1]:
                    place.on_planes(s, update(l))
                waiting[2 * l + 1] = []

    for b in range(rows // BLOCK):
        rs = slice(b * BLOCK, (b + 1) * BLOCK)

        def body(j, _):
            at = pl.ds(pl.multiple_of(j * TILE, TILE), TILE)
            mask = lax.broadcasted_iota(jnp.int32, (BLOCK, 1), 0) < live - b * BLOCK
            act[rs, at] = jnp.where(mask, resid[rs, at], 0.0).astype(jnp.bfloat16)
            return 0

        lax.fori_loop(0, width // TILE, body, 0)
        pltpu.make_async_copy(act.at[rs], out_ref.at[rs], out_sem.at[b]).start()

    count = len_ref[0]
    for k in range(1, n):
        count = count + len_ref[k]
    loss_ref[...] = losses.end() / count.astype(jnp.float32)

    rot.drain()
    for gather in gathers:
        gather.drain()
    for exchanged in [tops, *vranges, losses]:
        exchanged.drain()
    for b in range(rows // BLOCK):
        rs = slice(b * BLOCK, (b + 1) * BLOCK)
        pltpu.make_async_copy(act.at[rs], out_ref.at[rs], out_sem.at[b]).wait()


def window(lengths, hidden, joined, rotation, layers):
    n = lengths.shape[0]
    rows, width = hidden.shape
    cols = joined.shape[0] // (2 * layers)
    channels = n * cols
    planes = n // 8
    f32, bf16 = jnp.float32, jnp.bfloat16
    dma = pltpu.SemaphoreType.DMA
    kinds = 2 + layers
    vmem = pl.BlockSpec(memory_space=pltpu.VMEM)
    return pl.pallas_call(
        functools.partial(window_kernel, n, layers),
        name="window",
        in_specs=[
            pl.BlockSpec(memory_space=pltpu.SMEM),
            vmem,
            vmem,
            pl.BlockSpec(memory_space=pl.ANY),
        ],
        out_specs=[pl.BlockSpec(memory_space=pl.ANY), vmem],
        out_shape=[
            jax.ShapeDtypeStruct((rows, width), bf16),
            jax.ShapeDtypeStruct((1, 128), f32),
        ],
        scratch_shapes=[
            pltpu.VMEM((n,) + rotation.shape, bf16),
            pltpu.VMEM((layers, n, cols, width), bf16),
            pltpu.VMEM((layers, n, cols, width), bf16),
            pltpu.VMEM((rows, width), f32),
            pltpu.VMEM((2 * layers * cols, width), f32),
            pltpu.VMEM((rows, width), bf16),
            pltpu.VMEM((rows, channels), f32),
            pltpu.VMEM((rows, channels), bf16),
            pltpu.VMEM((1, channels), f32),
            pltpu.VMEM((rows, 1), f32),
            pltpu.VMEM((rows, 1), f32),
            pltpu.VMEM((rows, 1), f32),
            pltpu.VMEM((8, layers, width), f32),
            pltpu.VMEM((planes, layers, width), f32),
            pltpu.VMEM((layers, 8, 1, channels), f32),
            pltpu.VMEM((layers, planes, 1, channels), f32),
            pltpu.VMEM((8, 1, 128), f32),
            pltpu.VMEM((planes, 1, 128), f32),
            dma,
            dma((rows // BLOCK,)),
            dma((5, n // 2)),
            dma((n,)),
            dma((2 * layers, 5, n // 2)),
            dma((2 * layers, n)),
            dma((kinds, 8)),
            dma((kinds, 8)),
            dma((kinds, planes)),
            dma((kinds, planes)),
        ],
        compiler_params=pltpu.CompilerParams(
            collective_id=3, has_side_effects=True, vmem_limit_bytes=FULL_VMEM
        ),
        cost_estimate=pl.CostEstimate(
            flops=2 * rows * width * (width + 2 * layers * channels),
            bytes_accessed=4 * rows * width,
            transcendentals=0,
        ),
    )(lengths, hidden, joined, rotation)


def fits(n, hidden, rotation, cols):
    return (
        n % 8 == 0
        and cols % CHUNK == 0
        and rotation.shape[0] % CHUNK == 0
        and (8 * rotation.shape[0]) % 128 == 0
        and (8 * cols) % 128 == 0
        and hidden.shape[0] % BLOCK == 0
        and rotation.shape[1] % TILE == 0
    )


def per_device(hidden, rotation, norm_gain, value_weight, output_weight, lengths):
    layers = norm_gain.shape[0]
    cols = value_weight.shape[2]
    own_len = lax.dynamic_slice_in_dim(lengths, lax.axis_index("dp"), 1)
    scaled = (norm_gain[:, :, None] * value_weight.astype(jnp.float32)).astype(jnp.bfloat16)
    width = rotation.shape[1]
    depth = value_weight.shape[1]
    joined = jnp.concatenate(
        [
            jnp.swapaxes(scaled, 1, 2).reshape(layers * cols, depth),
            output_weight.reshape(layers * cols, depth),
        ],
        axis=0,
    )
    n = lax.axis_size("dp")
    if fits(n, hidden, rotation, cols):
        out, loss = window(lengths, hidden, joined, rotation, layers)
        return (out, loss[0, 0])
    rotation_full = lax.all_gather(rotation, "dp", axis=0, tiled=True)
    value_q, rotated_o, tops = rotate_weights(
        joined, rotation_full, layers * cols, layers * cols, layers
    )
    tops = exchange(tops, n, 0)
    output_q = [
        fake_quant(
            rotated_o[l * cols : (l + 1) * cols], tops[l : l + 1] / 7.0 + EPS_SCALE
        ).astype(jnp.bfloat16)
        for l in range(layers)
    ]
    value_all = lax.all_gather(value_q, "dp", axis=0, tiled=False)
    output_all = []
    for l in range(layers):
        before = output_all[l - 1] if l > 0 else value_all
        local_o, _ = lax.optimization_barrier((output_q[l], before))
        output_all.append(lax.all_gather(local_o, "dp", axis=0, tiled=True))
    resid, act, msq, aerr = first_pass(hidden, rotation_full)
    loss = jnp.zeros((), jnp.float32)
    for l in range(layers):
        mixed, top = mix_pass(own_len, act, value_all, l, cols)
        vrange = exchange(top, n, 1)
        last = l == layers - 1
        res = update_pass(own_len, mixed, vrange, output_all[l], resid, msq, aerr, last)
        loss = loss + jnp.sum(res[0])
        if last:
            out = res[1]
        else:
            resid, act, msq, aerr = res[1:]
    count = jnp.sum(lengths).astype(jnp.float32)
    loss = exchange(jnp.full((1, 128), loss, jnp.float32), n, 2, total=True)[0, 0]
    return (out, loss / count)


def solution(mesh):
    return jax.shard_map(
        per_device,
        mesh=mesh,
        in_specs=(P("dp", None), P("dp", None), P(), P(None, None, "dp"), P(None, "dp", None), P()),
        out_specs=(P("dp", None), P()),
        check_vma=False,
    )
```

```python
import functools

import jax
import jax.numpy as jnp
from jax import lax
from jax.experimental import pallas as pl
from jax.experimental.pallas import tpu as pltpu
from jax.sharding import PartitionSpec as P

BLOCK = 256
CHUNK = 16
TILE = 512
VMEM_LIMIT = 60 * 1024 * 1024

EPS_NORM = 1e-06
EPS_SCALE = 1e-06
CLIP_RATIO = 0.9
POLY = (0.9999997571452157, -2.579687436847881, 2.6673586060553345, -1.5145036626283546, 0.48039577352173)


def soft_round(values):
    r = values - jnp.round(values)
    u = r * r
    p = jnp.float32(POLY[-1])
    for c in POLY[-2::-1]:
        p = p * u + jnp.float32(c)
    return values - p * (r - 4.0 * (r * u))


def fake_quant(values, step_size):
    inv = 1.0 / step_size
    return soft_round(jnp.clip(values * inv, -8.0, 7.0)) * step_size


def exchange_kernel(n, total, x_ref, out_ref, slots, send_sem, recv_sem):
    me = lax.axis_index("dp")
    barrier = pltpu.get_barrier_semaphore()

    def greet(k, _):
        pl.semaphore_signal(
            barrier,
            inc=1,
            device_id=(lax.rem(me + k, n),),
            device_id_type=pl.DeviceIdType.MESH,
        )
        return 0

    lax.fori_loop(1, n, greet, 0)
    pl.semaphore_wait(barrier, n - 1)

    def copy_to(peer, slot):
        return pltpu.make_async_remote_copy(
            src_ref=x_ref,
            dst_ref=slots.at[slot],
            send_sem=send_sem.at[peer],
            recv_sem=recv_sem.at[slot],
            device_id=(peer,),
            device_id_type=pl.DeviceIdType.MESH,
        )

    def push(k, _):
        copy_to(lax.rem(me + k, n), me).start()
        return 0

    lax.fori_loop(1, n, push, 0)
    slots[me] = x_ref[...]

    def settle(k, _):
        peer = lax.rem(me + k, n)
        copy = copy_to(peer, peer)
        copy.wait_send()
        copy.wait_recv()
        return 0

    lax.fori_loop(1, n, settle, 0)

    def fold(k, acc):
        return acc + slots[k] if total else jnp.maximum(acc, slots[k])

    out_ref[...] = lax.fori_loop(1, n, fold, slots[0])


def exchange(x, n, collective_id, total=False):
    return pl.pallas_call(
        functools.partial(exchange_kernel, n, total),
        name="exchange",
        in_specs=[pl.BlockSpec(memory_space=pltpu.VMEM)],
        out_specs=pl.BlockSpec(memory_space=pltpu.VMEM),
        out_shape=jax.ShapeDtypeStruct(x.shape, x.dtype),
        scratch_shapes=[
            pltpu.VMEM((n,) + x.shape, x.dtype),
            pltpu.SemaphoreType.DMA((n,)),
            pltpu.SemaphoreType.DMA((n,)),
        ],
        compiler_params=pltpu.CompilerParams(
            collective_id=collective_id, has_side_effects=True, vmem_limit_bytes=VMEM_LIMIT
        ),
        cost_estimate=pl.CostEstimate(flops=0, bytes_accessed=30_000_000, transcendentals=0),
    )(x)


def weight_kernel(v_rows, o_rows, layers, w_ref, r_ref, vq_ref, o_ref, top_ref, acc):
    j = pl.program_id(0)
    n = r_ref.shape[1]
    at = pl.ds(pl.multiple_of(j * n, n), n)
    prod = jnp.dot(w_ref[...], r_ref[...], preferred_element_type=jnp.float32)
    acc[:, at] = prod[:v_rows]
    o_ref[...] = prod[v_rows:]
    per = o_rows // layers
    for l in range(layers):
        lo = v_rows + l * per
        top_ref[l : l + 1, :] = jnp.max(jnp.abs(prod[lo : lo + per]), axis=0, keepdims=True)

    @pl.when(j == pl.num_programs(0) - 1)
    def _():
        def body(i, _):
            rows = pl.ds(pl.multiple_of(i * CHUNK, CHUNK), CHUNK)
            x = acc[rows, :]
            step = jnp.max(jnp.abs(x), axis=1, keepdims=True) / 7.0 + EPS_SCALE
            vq_ref[rows, :] = fake_quant(x, step).astype(jnp.bfloat16)
            return 0

        lax.fori_loop(0, v_rows // CHUNK, body, 0)


def rotate_weights(joined, rotation, v_rows, o_rows, layers):
    width = rotation.shape[1]
    depth = rotation.shape[0]
    return pl.pallas_call(
        functools.partial(weight_kernel, v_rows, o_rows, layers),
        name="rotate_weights",
        grid=(width // TILE,),
        in_specs=[
            pl.BlockSpec(joined.shape, lambda j: (0, 0)),
            pl.BlockSpec((depth, TILE), lambda j: (0, j)),
        ],
        out_specs=[
            pl.BlockSpec((v_rows, width), lambda j: (0, 0)),
            pl.BlockSpec((o_rows, TILE), lambda j: (0, j)),
            pl.BlockSpec((layers, TILE), lambda j: (0, j)),
        ],
        out_shape=[
            jax.ShapeDtypeStruct((v_rows, width), jnp.bfloat16),
            jax.ShapeDtypeStruct((o_rows, width), jnp.float32),
            jax.ShapeDtypeStruct((layers, width), jnp.float32),
        ],
        scratch_shapes=[pltpu.VMEM((v_rows, width), jnp.float32)],
        compiler_params=pltpu.CompilerParams(vmem_limit_bytes=VMEM_LIMIT),
        cost_estimate=pl.CostEstimate(
            flops=2 * joined.shape[0] * depth * width,
            bytes_accessed=2 * depth * width,
            transcendentals=0,
        ),
    )(joined, rotation)


def norm_rows(resid_ref, act_ref, msq_ref, aerr_ref):
    width = resid_ref.shape[1]

    def body(i, _):
        rows = pl.ds(pl.multiple_of(i * CHUNK, CHUNK), CHUNK)
        x = resid_ref[rows, :]
        mean_sq = jnp.sum(x * x, axis=1, keepdims=True) * (1.0 / width)
        inv = lax.rsqrt(mean_sq + EPS_NORM)
        step = CLIP_RATIO * (jnp.max(jnp.abs(x), axis=1, keepdims=True) * inv) / 7.0 + EPS_SCALE
        normed = x * inv
        act = fake_quant(normed, step)
        diff = act - normed
        act_ref[rows, :] = act.astype(jnp.bfloat16)
        msq_ref[rows, :] = mean_sq
        aerr_ref[rows, :] = jnp.sum(diff * diff, axis=1, keepdims=True)
        return 0

    lax.fori_loop(0, resid_ref.shape[0] // CHUNK, body, 0)


def first_kernel(h_ref, r_ref, resid_ref, act_ref, msq_ref, aerr_ref):
    def body(j, _):
        at = pl.ds(pl.multiple_of(j * TILE, TILE), TILE)
        resid_ref[:, at] = jnp.dot(h_ref[...], r_ref[:, at], preferred_element_type=jnp.float32)
        return 0

    lax.fori_loop(0, r_ref.shape[1] // TILE, body, 0)
    norm_rows(resid_ref, act_ref, msq_ref, aerr_ref)


def rows_spec(width):
    return pl.BlockSpec((BLOCK, width), lambda i, *_: (i, 0))


def whole_spec(shape):
    return pl.BlockSpec(shape, lambda i, *_: (0, 0), pipeline_mode=pl.Buffered(1))


def act_shapes(rows, width):
    return [
        jax.ShapeDtypeStruct((rows, width), jnp.float32),
        jax.ShapeDtypeStruct((rows, width), jnp.bfloat16),
        jax.ShapeDtypeStruct((rows, 1), jnp.float32),
        jax.ShapeDtypeStruct((rows, 1), jnp.float32),
    ]


def first_pass(hidden, rotation):
    rows, depth = hidden.shape
    width = rotation.shape[1]
    return pl.pallas_call(
        first_kernel,
        name="rotate_hidden",
        grid=(rows // BLOCK,),
        in_specs=[rows_spec(depth), whole_spec(rotation.shape)],
        out_specs=[rows_spec(width), rows_spec(width), rows_spec(1), rows_spec(1)],
        out_shape=act_shapes(rows, width),
        compiler_params=pltpu.CompilerParams(vmem_limit_bytes=VMEM_LIMIT),
        cost_estimate=pl.CostEstimate(
            flops=2 * rows * depth * width,
            bytes_accessed=2 * depth * width + 8 * rows * width,
            transcendentals=0,
        ),
    )(hidden, rotation)


def mix_kernel(len_ref, act_ref, v_ref, mixed_ref, top_ref):
    i = pl.program_id(0)
    tile = 256
    live = len_ref[0] - i * BLOCK
    mask = lax.broadcasted_iota(jnp.int32, (BLOCK, 1), 0) < live

    @pl.when(i == 0)
    def _():
        top_ref[...] = jnp.zeros_like(top_ref)

    cols = v_ref.shape[1]
    group = tile // cols

    def body(j, _):
        at = pl.ds(pl.multiple_of(j * tile, tile), tile)
        part = v_ref[pl.ds(j * group, group)]
        prod = lax.dot_general(
            act_ref[...],
            part.reshape(tile, part.shape[2]),
            (((1,), (1,)), ((), ())),
            preferred_element_type=jnp.float32,
        )
        mixed_ref[:, at] = prod
        peak = jnp.max(jnp.where(mask, jnp.abs(prod), 0.0), axis=0, keepdims=True)
        top_ref[:, at] = jnp.maximum(top_ref[:, at], peak)
        return 0

    lax.fori_loop(0, v_ref.shape[0] // group, body, 0)


def mix_pass(own_len, act, gathered, layer, cols):
    rows, width = act.shape
    n = gathered.shape[0]
    channels = n * cols
    if cols % 16 == 0:
        values = gathered
        spec = pl.BlockSpec(
            (n, cols, width), lambda i, *_: (0, layer, 0), pipeline_mode=pl.Buffered(1)
        )
    else:
        values = gathered[:, layer * cols : (layer + 1) * cols].reshape(-1, 128, width)
        spec = pl.BlockSpec(values.shape, lambda i, *_: (0, 0, 0), pipeline_mode=pl.Buffered(1))
    return pl.pallas_call(
        mix_kernel,
        name="mix",
        grid_spec=pltpu.PrefetchScalarGridSpec(
            num_scalar_prefetch=1,
            grid=(rows // BLOCK,),
            in_specs=[rows_spec(width), spec],
            out_specs=[
                rows_spec(channels),
                pl.BlockSpec((1, channels), lambda i, *_: (0, 0)),
            ],
        ),
        out_shape=[
            jax.ShapeDtypeStruct((rows, channels), jnp.float32),
            jax.ShapeDtypeStruct((1, channels), jnp.float32),
        ],
        compiler_params=pltpu.CompilerParams(vmem_limit_bytes=VMEM_LIMIT),
        cost_estimate=pl.CostEstimate(
            flops=2 * rows * channels * width,
            bytes_accessed=2 * channels * width + 4 * rows * width,
            transcendentals=0,
        ),
    )(own_len, act, values)


def update_kernel(last, len_ref, mixed_ref, vrange_ref, o_ref, resid_ref, msq_ref, aerr_ref, *rest):
    if last:
        loss_ref, out_ref, mix_buf = rest
    else:
        loss_ref, new_ref, act_ref, nmsq_ref, naerr_ref, mix_buf = rest
    live = len_ref[0] - pl.program_id(0) * BLOCK
    mask = lax.broadcasted_iota(jnp.int32, (BLOCK, 1), 0) < live
    step = CLIP_RATIO * vrange_ref[...] / 7.0 + EPS_SCALE

    def quant(i, _):
        rows = pl.ds(pl.multiple_of(i * CHUNK, CHUNK), CHUNK)
        x = mixed_ref[rows, :]
        mix = fake_quant(x, step)
        diff = mix - x
        mix_buf[rows, :] = mix.astype(jnp.bfloat16)
        loss_ref[rows, :] = jnp.sum(diff * diff, axis=1, keepdims=True)
        return 0

    lax.fori_loop(0, BLOCK // CHUNK, quant, 0)
    loss_ref[...] = jnp.where(mask, msq_ref[...] * (aerr_ref[...] + loss_ref[...]), 0.0)

    def body(j, _):
        at = pl.ds(pl.multiple_of(j * TILE, TILE), TILE)
        new = resid_ref[:, at] + jnp.dot(
            mix_buf[...], o_ref[:, at], preferred_element_type=jnp.float32
        )
        if last:
            out_ref[:, at] = jnp.where(mask, new, 0.0).astype(jnp.bfloat16)
        else:
            new_ref[:, at] = new
        return 0

    lax.fori_loop(0, o_ref.shape[1] // TILE, body, 0)
    if not last:
        norm_rows(new_ref, act_ref, nmsq_ref, naerr_ref)


def update_pass(own_len, mixed, vrange, outputs, resid, msq, aerr, last):
    rows, width = resid.shape
    channels = mixed.shape[1]
    out_specs = [rows_spec(1)]
    out_shape = [jax.ShapeDtypeStruct((rows, 1), jnp.float32)]
    if last:
        out_specs.append(rows_spec(width))
        out_shape.append(jax.ShapeDtypeStruct((rows, width), jnp.bfloat16))
    else:
        out_specs += [rows_spec(width), rows_spec(width), rows_spec(1), rows_spec(1)]
        out_shape += act_shapes(rows, width)
    return pl.pallas_call(
        functools.partial(update_kernel, last),
        name="update",
        grid_spec=pltpu.PrefetchScalarGridSpec(
            num_scalar_prefetch=1,
            grid=(rows // BLOCK,),
            in_specs=[
                rows_spec(channels),
                whole_spec((1, channels)),
                whole_spec(outputs.shape),
                rows_spec(width),
                rows_spec(1),
                rows_spec(1),
            ],
            out_specs=out_specs,
            scratch_shapes=[pltpu.VMEM((BLOCK, channels), jnp.bfloat16)],
        ),
        out_shape=out_shape,
        compiler_params=pltpu.CompilerParams(vmem_limit_bytes=VMEM_LIMIT),
        cost_estimate=pl.CostEstimate(
            flops=2 * rows * channels * width,
            bytes_accessed=2 * channels * width + 12 * rows * width,
            transcendentals=0,
        ),
    )(own_len, mixed, vrange, outputs, resid, msq, aerr)


MESH_ID = pl.DeviceIdType.MESH
FULL_VMEM = 67043328
STRIP = 128
ROT_TILE = 256
LANES = 128
HALVES = 2
CROSS_TENTHS = 2
ROT_STEP, ROT_GAP = 6.0, 12.0
STEP, GAP = 6.0, 17.0


class Place:
    def __init__(self, n):
        me = lax.axis_index("dp")
        core = lax.rem(me, 2)
        self.me, self.planes, self.core = me, n // 8, core
        self.z = me // 8
        self.stride2 = 2 + 2 * core
        self.stride3 = 4 - 2 * core
        self.bit2 = lax.rem(me // self.stride2, 2)
        self.bit3 = lax.rem(me // self.stride3, 2)
        self.to = [
            me + 8,
            me - 8,
            me + self.stride2 * (1 - 2 * self.bit2),
            me + self.stride3 * (1 - 2 * self.bit3),
            me + 1 - 2 * core,
        ]

    def origin(self, plane, flip2, flip3):
        bit2 = 1 - self.bit2 if flip2 else self.bit2
        bit3 = 1 - self.bit3 if flip3 else self.bit3
        return 8 * plane + self.core + self.stride2 * bit2 + self.stride3 * bit3

    def at_distance(self, s):
        if s == 0:
            return [(self.z, None)]
        return [(self.z - s, self.z >= s), (self.z + s, self.z + s < self.planes)]

    def on_planes(self, s, piece):
        if s == 0:
            piece(self.z)
            return

        def body(k, _):
            plane = self.z - s + 2 * s * k
            pl.when(jnp.logical_and(plane >= 0, plane < self.planes))(lambda: piece(plane))
            return 0

        lax.fori_loop(0, 2, body, 0)

    def greet(self):
        barrier = pltpu.get_barrier_semaphore()
        peers = [8 * self.z + lax.rem(self.me + k, 8) for k in range(1, 8)]
        peers += [lax.rem(self.me + 8 * k, 8 * self.planes) for k in range(1, self.planes)]
        for peer in peers:
            pl.semaphore_signal(barrier, inc=1, device_id=(peer,), device_id_type=MESH_ID)
        pl.semaphore_wait(barrier, len(peers))


def run_if(cond, fn):
    if cond is None:
        fn()
    else:
        pl.when(cond)(fn)


def start(copy):
    copy.start()


def sent(copy):
    copy.wait_send()


class Gather:
    def __init__(self, place, buf, send_sem, recv_sem, columns=slice(None)):
        self.place, self.buf, self.send_sem, self.recv_sem = place, buf, send_sem, recv_sem
        self.columns = columns

    def copy(self, o, d):
        return pltpu.make_async_remote_copy(
            src_ref=self.buf.at[o, :, self.columns],
            dst_ref=self.buf.at[o, :, self.columns],
            send_sem=self.send_sem.at[d, o // 2],
            recv_sem=self.recv_sem.at[o],
            device_id=(self.place.to[d],),
            device_id_type=MESH_ID,
        )

    def arrived(self, o):
        self.copy(o, 4).wait_recv()

    def up(self, o, act):
        pl.when(self.place.z < self.place.planes - 1)(lambda: act(self.copy(o, 0)))

    def down(self, o, act):
        pl.when(self.place.z > 0)(lambda: act(self.copy(o, 1)))

    def own(self, act=start):
        o = self.place.me
        self.up(o, act)
        self.down(o, act)
        for d in (2, 3, 4):
            act(self.copy(o, d))

    def line(self, s, act=start):
        for k, (plane, cond) in enumerate(self.place.at_distance(s)):

            def go(k=k, plane=plane):
                o = self.place.origin(plane, 0, 0)
                if act is start:
                    self.arrived(o)
                (self.up if k == 0 else self.down)(o, act)
                for d in (2, 3, 4):
                    act(self.copy(o, d))

            run_if(cond, go)

    def second(self, s, act=start):
        for plane, cond in self.place.at_distance(s):

            def go(plane=plane):
                o = self.place.origin(plane, 1, 0)
                if act is start:
                    self.arrived(o)
                for d in (3, 4):
                    act(self.copy(o, d))

            run_if(cond, go)

    def third(self, s, act=start):
        for plane, cond in self.place.at_distance(s):

            def go(plane=plane):
                for flip2 in (0, 1):
                    o = self.place.origin(plane, flip2, 1)
                    if act is start:
                        self.arrived(o)
                    act(self.copy(o, 4))

            run_if(cond, go)

    def other_core(self, s):
        for plane, cond in self.place.at_distance(s):

            def go(plane=plane):
                def body(q, _):
                    self.arrived(8 * plane + 2 * q + 1 - self.place.core)
                    return 0

                lax.fori_loop(0, 4, body, 0)

            run_if(cond, go)

    def events(self):
        planes = self.place.planes
        out = [(0, self.own, None)]
        for t in range(1, planes + 2):
            if t < planes:
                out.append((t, functools.partial(self.line, t), None))
            if t < planes + 1:
                out.append((t, functools.partial(self.second, t - 1), None))
            if t >= 2:
                out.append((t, functools.partial(self.third, t - 2), None))
                out.append((t + 0.3, functools.partial(self.other_core, t - 2), t - 2))
        return out

    def drain(self):
        self.own(sent)
        for s in range(self.place.planes):
            if s:
                self.line(s, sent)
            self.second(s, sent)
            self.third(s, sent)


class Cross(Gather):
    def second(self, act=start):
        o = self.place.origin(self.place.z, 1, 0)
        if act is start:
            self.arrived(o)
        self.up(o, act)
        self.down(o, act)
        for d in (3, 4):
            act(self.copy(o, d))

    def third(self, act=start):
        for flip2 in (0, 1):
            o = self.place.origin(self.place.z, flip2, 1)
            if act is start:
                self.arrived(o)
            self.up(o, act)
            self.down(o, act)
            act(self.copy(o, 4))

    def line(self, s, act=start):
        for k, (plane, cond) in enumerate(self.place.at_distance(s)):

            def go(k=k, plane=plane):
                def body(q, _):
                    o = 8 * plane + 2 * q + self.place.core
                    if act is start:
                        self.arrived(o)
                    (self.up if k == 0 else self.down)(o, act)
                    act(self.copy(o, 4))
                    return 0

                lax.fori_loop(0, 4, body, 0)

            run_if(cond, go)

    def events(self):
        out = [(0, self.own, None), (0.5, self.second, None), (1.2, self.third, None)]
        out.append((1.8, functools.partial(self.other_core, 0), 0))
        for s in range(1, self.place.planes):
            out.append((1.2 + s, functools.partial(self.line, s), None))
            out.append((2.3 + s, functools.partial(self.other_core, s), s))
        return out

    def drain(self):
        self.own(sent)
        self.second(sent)
        self.third(sent)
        for s in range(1, self.place.planes):
            self.line(s, sent)


class Exchange:
    def __init__(self, place, total, near, far, near_send, near_recv, far_send, far_recv):
        self.place, self.total, self.near, self.far = place, total, near, far
        self.sems = (near_send, near_recv, far_send, far_recv)
        self.spot = lax.rem(place.me, 8)

    def near_copy(self, k, slot):
        spot = lax.rem(self.spot + k, 8)
        return pltpu.make_async_remote_copy(
            src_ref=self.near.at[slot],
            dst_ref=self.near.at[slot],
            send_sem=self.sems[0].at[k],
            recv_sem=self.sems[1].at[slot],
            device_id=(8 * self.place.z + spot,),
            device_id_type=MESH_ID,
        )

    def far_copy(self, k, slot):
        plane = lax.rem(self.place.z + k, self.place.planes)
        return pltpu.make_async_remote_copy(
            src_ref=self.far.at[slot],
            dst_ref=self.far.at[slot],
            send_sem=self.sems[2].at[k],
            recv_sem=self.sems[3].at[slot],
            device_id=(8 * plane + self.spot,),
            device_id_type=MESH_ID,
        )

    def fold(self, slots, count):
        acc = slots[0]
        for k in range(1, count):
            acc = acc + slots[k] if self.total else jnp.maximum(acc, slots[k])
        return acc

    def begin(self, value):
        self.near[self.spot] = value
        for k in range(1, 8):
            self.near_copy(k, self.spot).start()

    def middle(self):
        for k in range(1, 8):
            self.near_copy(k, lax.rem(self.spot + k, 8)).wait_recv()
        self.far[self.place.z] = self.fold(self.near, 8)
        for k in range(1, self.place.planes):
            self.far_copy(k, self.place.z).start()

    def end(self):
        for k in range(1, self.place.planes):
            self.far_copy(k, lax.rem(self.place.z + k, self.place.planes)).wait_recv()
        return self.fold(self.far, self.place.planes)

    def drain(self):
        for k in range(1, 8):
            self.near_copy(k, self.spot).wait_send()
        for k in range(1, self.place.planes):
            self.far_copy(k, self.place.z).wait_send()


class Plan:
    def __init__(self):
        self.now, self.waits, self.work, self.count = 0.0, [], [], 0

    def wait(self, when, action):
        self.count += 1
        self.waits.append((when, self.count, action))

    def compute(self, rank, cost, action):
        self.count += 1
        self.work.append((rank, self.count, cost, action))

    def run(self):
        while self.waits or self.work:
            self.waits.sort(key=lambda w: w[:2])
            self.work.sort(key=lambda w: w[:2])
            if self.waits and (not self.work or self.waits[0][0] <= self.now):
                when, _, action = self.waits.pop(0)
                self.now = max(self.now, when)
                action()
            else:
                _, _, cost, action = self.work.pop(0)
                action()
                self.now += cost


def soft_parts(scaled):
    v = jnp.clip(scaled, -8.0, 7.0)
    r = v - jnp.round(v)
    u = r * r
    p = jnp.float32(POLY[-1])
    for c in POLY[-2::-1]:
        p = p * u + jnp.float32(c)
    return v - (p * (1.0 - 4.0 * u)) * r


def window_kernel(n, layers, *refs):
    len_ref, h_ref, w_ref, r_ref, out_ref, loss_ref = refs[:6]
    (rbuf, vbuf, obuf, resid, wacc, act, mixed, mixq, top, msq, aerr, lossrow, size, scale) = refs[6:20]
    (ntops, ftops, ntop, ftop, nloss, floss) = refs[20:26]
    (local_sem, out_sem, rsend, rrecv, wsend, wrecv, xns, xnr, xfs, xfr) = refs[26:]
    place = Place(n)
    planes = place.planes
    rows, width = resid.shape
    cols = vbuf.shape[2]
    channels = n * cols
    depth = 8 * r_ref.shape[0]
    lanes = 8 * cols
    half = width // HALVES
    live = len_ref[place.me]
    strips = rows // STRIP

    mine = pltpu.make_async_copy(r_ref, rbuf.at[place.me], local_sem)
    mine.start()
    place.greet()
    mine.wait()

    def both(buf, send_sem, recv_sem, lo, span):
        cut = span * CROSS_TENTHS // 10 // 128 * 128
        return (
            Gather(place, buf, send_sem.at[0], recv_sem.at[0], pl.ds(lo, span - cut)),
            Cross(place, buf, send_sem.at[1], recv_sem.at[1], pl.ds(lo + span - cut, cut)),
        )

    rots = [both(rbuf, rsend.at[q], rrecv.at[q], q * half, half) for q in range(HALVES)]
    gathers = []
    for l in range(layers):
        gathers.append(both(vbuf.at[l], wsend.at[2 * l], wrecv.at[2 * l], 0, width))
        gathers.append(both(obuf.at[l], wsend.at[2 * l + 1], wrecv.at[2 * l + 1], 0, width))

    def make(i, total, near, far):
        return Exchange(place, total, near, far, xns.at[i], xnr.at[i], xfs.at[i], xfr.at[i])

    tops = make(0, False, ntops, ftops)
    vranges = [make(1 + l, False, ntop.at[l], ftop.at[l]) for l in range(layers)]
    losses = make(1 + layers, True, nloss, floss)
    vrows = layers * cols

    def product(q, left, total, first):
        def piece(plane):
            ks = pl.ds(pl.multiple_of(plane * depth, 128), depth)

            def body(j, _):
                at = pl.ds(pl.multiple_of(q * half + j * ROT_TILE, ROT_TILE), ROT_TILE)
                part = rbuf[pl.ds(8 * plane, 8), :, at].reshape(depth, ROT_TILE)
                prod = jnp.dot(left[:, ks], part, preferred_element_type=jnp.float32)
                if first:
                    total[:, at] = prod
                else:
                    total[:, at] += prod
                return 0

            lax.fori_loop(0, half // ROT_TILE, body, 0)

        return piece

    def quantize_values():
        for l in range(layers):
            for i in range(cols // CHUNK):
                x = wacc[l * cols + i * CHUNK : l * cols + (i + 1) * CHUNK, :]
                step = jnp.max(jnp.abs(x), axis=1, keepdims=True) / 7.0 + EPS_SCALE
                vbuf[l, place.me, i * CHUNK : (i + 1) * CHUNK, :] = fake_quant(x, step).astype(jnp.bfloat16)

    def begin_tops():
        peaks = [
            jnp.max(jnp.abs(wacc[vrows + l * cols : vrows + (l + 1) * cols, :]), axis=0, keepdims=True)
            for l in range(layers)
        ]
        tops.begin(jnp.concatenate(peaks, axis=0))

    def quantize_outputs():
        peaks = tops.end()
        for l in range(layers):
            lo = vrows + l * cols
            obuf[l, place.me] = fake_quant(
                wacc[lo : lo + cols, :], peaks[l : l + 1] / 7.0 + EPS_SCALE
            ).astype(jnp.bfloat16)

    def norm(p):
        at = pl.ds(pl.multiple_of(p * STRIP, STRIP), STRIP)
        total = jnp.zeros((STRIP, LANES), jnp.float32)
        peak = jnp.zeros((STRIP, LANES), jnp.float32)
        for j in range(width // LANES):
            x = resid[at, j * LANES : (j + 1) * LANES]
            total = total + x * x
            peak = jnp.maximum(peak, jnp.abs(x))
        mean_sq = jnp.sum(total, axis=1, keepdims=True) * (1.0 / width)
        inv = lax.rsqrt(mean_sq + EPS_NORM)
        step = CLIP_RATIO * (jnp.max(peak, axis=1, keepdims=True) * inv) / 7.0 + EPS_SCALE
        msq[at, :] = mean_sq
        size[at, :] = step
        scale[at, :] = inv / step
        wide_step = jnp.broadcast_to(size[at, :], (STRIP, LANES))
        wide_scale = jnp.broadcast_to(scale[at, :], (STRIP, LANES))
        err = jnp.zeros((STRIP, LANES), jnp.float32)
        for j in range(width // LANES):
            scaled = resid[at, j * LANES : (j + 1) * LANES] * wide_scale
            q = soft_parts(scaled)
            act[at, j * LANES : (j + 1) * LANES] = (q * wide_step).astype(jnp.bfloat16)
            diff = q - scaled
            err = err + diff * diff
        aerr[at, :] = jnp.sum(err, axis=1, keepdims=True) * (size[at, :] * size[at, :])

    def norm_strips(lo, hi):
        def body(p, _):
            norm(p)
            return 0

        lax.fori_loop(lo, hi, body, 0)

    def mix(l):
        def piece(plane):
            at = pl.ds(pl.multiple_of(plane * lanes, 128), lanes)
            part = vbuf[l, pl.ds(8 * plane, 8)].reshape(lanes, width)
            peak = jnp.zeros((1, lanes), jnp.float32)
            for b in range(rows // BLOCK):
                rs = slice(b * BLOCK, (b + 1) * BLOCK)
                prod = lax.dot_general(
                    act[rs, :], part, (((1,), (1,)), ((), ())), preferred_element_type=jnp.float32
                )
                mixed[rs, at] = prod
                mask = lax.broadcasted_iota(jnp.int32, (BLOCK, 1), 0) < live - b * BLOCK
                peak = jnp.maximum(
                    peak, jnp.max(jnp.where(mask, jnp.abs(prod), 0.0), axis=0, keepdims=True)
                )
            top[:, at] = peak

        return piece

    def quantize_mixed(l, lo, hi):
        def body(p, _):
            at = pl.ds(pl.multiple_of(p * STRIP, STRIP), STRIP)
            err = jnp.zeros((STRIP, LANES), jnp.float32)
            for j in range(channels // LANES):
                cut = slice(j * LANES, (j + 1) * LANES)
                step = CLIP_RATIO * top[:, cut] / 7.0 + EPS_SCALE
                inv = 1.0 / step
                x = mixed[at, cut]
                q = soft_parts(x * inv) * step
                mixq[at, cut] = q.astype(jnp.bfloat16)
                diff = q - x
                err = err + diff * diff
            mask = lax.broadcasted_iota(jnp.int32, (STRIP, 1), 0) < live - p * STRIP
            both = aerr[at, :] + jnp.sum(err, axis=1, keepdims=True)
            row = jnp.where(mask, msq[at, :] * both, 0.0)
            if l == 0:
                lossrow[at, :] = row
            else:
                lossrow[at, :] += row
            return 0

        lax.fori_loop(lo, hi, body, 0)

    def update(l):
        def piece(plane):
            ks = pl.ds(pl.multiple_of(plane * lanes, 128), lanes)

            def body(j, _):
                at = pl.ds(pl.multiple_of(j * TILE, TILE), TILE)
                part = obuf[l, pl.ds(8 * plane, 8), :, at].reshape(lanes, TILE)
                resid[:, at] += jnp.dot(mixq[:, ks], part, preferred_element_type=jnp.float32)
                return 0

            lax.fori_loop(0, width // TILE, body, 0)

        return piece

    plan = Plan()
    held = [[] for _ in gathers]
    open_ = [False] * len(gathers)

    def gather_waits(pair, base, step, arrived):
        here = [0] * planes
        for gather in pair[::-1]:
            for t, action, distance in gather.events():

                def go(action=action, distance=distance):
                    action()
                    if distance is not None:
                        here[distance] += 1
                        if here[distance] == len(pair):
                            arrived(distance)

                plan.wait(base + step * t, go)

    def rotated(q):
        def arrived(s):
            plan.compute(0, 0.3, lambda: (place.on_planes(s, product(q, w_ref, wacc, s == 0)), weights_done()))
            plan.compute(1, 2.2, lambda: (place.on_planes(s, product(q, h_ref, resid, s == 0)), hidden_done()))

        return arrived

    counts = {"w": 0, "h": 0, "norm": [0] * layers, "mix": [0] * layers, "quant": [0] * layers, "upd": [0] * layers}

    def weights_done():
        counts["w"] += 1
        if counts["w"] < HALVES * planes:
            return
        quantize_values()
        base = plan.now
        gather_waits(gathers[0], base, STEP, shards(0))
        plan.wait(base + 0.1, begin_tops)
        plan.wait(base + 4.0, tops.middle)

        def outputs():
            quantize_outputs()
            for g in range(1, 2 * layers):
                gather_waits(gathers[g], max(plan.now, base + GAP * g), STEP, shards(g))

        plan.wait(base + 8.0, outputs)

    def hidden_done():
        counts["h"] += 1
        if counts["h"] == HALVES * planes:
            start_norm(0)

    def start_norm(l):
        for p in range(0, strips, 2):
            plan.compute(2, 3.0, lambda p=p: (norm_strips(p, p + 2), norm_done(l)))

    def norm_done(l):
        counts["norm"][l] += 2
        if counts["norm"][l] == strips:
            release(2 * l)

    def release(g):
        open_[g] = True
        for s in held[g]:
            add_piece(g, s)
        held[g] = []

    def shards(g):
        def arrived(s):
            if open_[g]:
                add_piece(g, s)
            else:
                held[g].append(s)

        return arrived

    def add_piece(g, s):
        l = g // 2
        if g % 2 == 0:
            plan.compute(3, 1.3, lambda: (place.on_planes(s, mix(l)), mix_done(l)))
        else:
            plan.compute(5, 1.9, lambda: (place.on_planes(s, update(l)), update_done(l)))

    def mix_done(l):
        counts["mix"][l] += 1
        if counts["mix"][l] < planes:
            return
        vranges[l].begin(top[...])
        plan.wait(plan.now + 4.0, vranges[l].middle)

        def end():
            top[...] = vranges[l].end()
            for p in range(0, strips, 2):
                plan.compute(4, 1.2, lambda p=p: (quantize_mixed(l, p, p + 2), quant_done(l)))

        plan.wait(plan.now + 8.0, end)

    def quant_done(l):
        counts["quant"][l] += 2
        if counts["quant"][l] < strips:
            return
        if l == layers - 1:
            losses.begin(jnp.broadcast_to(jnp.sum(lossrow[...], axis=0, keepdims=True), (1, 128)))
            plan.wait(plan.now + 4.0, losses.middle)
        release(2 * l + 1)

    def update_done(l):
        counts["upd"][l] += 1
        if counts["upd"][l] == planes and l < layers - 1:
            start_norm(l + 1)

    for q in range(HALVES):
        gather_waits(rots[q], q * ROT_GAP, ROT_STEP, rotated(q))
    plan.run()

    for b in range(rows // BLOCK):
        rs = slice(b * BLOCK, (b + 1) * BLOCK)

        def body(j, _):
            at = pl.ds(pl.multiple_of(j * TILE, TILE), TILE)
            mask = lax.broadcasted_iota(jnp.int32, (BLOCK, 1), 0) < live - b * BLOCK
            act[rs, at] = jnp.where(mask, resid[rs, at], 0.0).astype(jnp.bfloat16)
            return 0

        lax.fori_loop(0, width // TILE, body, 0)
        pltpu.make_async_copy(act.at[rs], out_ref.at[rs], out_sem.at[b]).start()

    count = len_ref[0]
    for k in range(1, n):
        count = count + len_ref[k]
    loss_ref[...] = losses.end() / count.astype(jnp.float32)

    for pair in rots + gathers:
        for gather in pair:
            gather.drain()
    for exchanged in [tops, *vranges, losses]:
        exchanged.drain()
    for b in range(rows // BLOCK):
        rs = slice(b * BLOCK, (b + 1) * BLOCK)
        pltpu.make_async_copy(act.at[rs], out_ref.at[rs], out_sem.at[b]).wait()


def window(lengths, hidden, joined, rotation, layers):
    n = lengths.shape[0]
    rows, width = hidden.shape
    cols = joined.shape[0] // (2 * layers)
    channels = n * cols
    planes = n // 8
    f32, bf16 = jnp.float32, jnp.bfloat16
    dma = pltpu.SemaphoreType.DMA
    kinds = 2 + layers
    vmem = pl.BlockSpec(memory_space=pltpu.VMEM)
    return pl.pallas_call(
        functools.partial(window_kernel, n, layers),
        name="window",
        in_specs=[
            pl.BlockSpec(memory_space=pltpu.SMEM),
            vmem,
            vmem,
            pl.BlockSpec(memory_space=pl.ANY),
        ],
        out_specs=[pl.BlockSpec(memory_space=pl.ANY), vmem],
        out_shape=[
            jax.ShapeDtypeStruct((rows, width), bf16),
            jax.ShapeDtypeStruct((1, 128), f32),
        ],
        scratch_shapes=[
            pltpu.VMEM((n,) + rotation.shape, bf16),
            pltpu.VMEM((layers, n, cols, width), bf16),
            pltpu.VMEM((layers, n, cols, width), bf16),
            pltpu.VMEM((rows, width), f32),
            pltpu.VMEM((2 * layers * cols, width), f32),
            pltpu.VMEM((rows, width), bf16),
            pltpu.VMEM((rows, channels), f32),
            pltpu.VMEM((rows, channels), bf16),
            pltpu.VMEM((1, channels), f32),
            pltpu.VMEM((rows, 1), f32),
            pltpu.VMEM((rows, 1), f32),
            pltpu.VMEM((rows, 1), f32),
            pltpu.VMEM((rows, 1), f32),
            pltpu.VMEM((rows, 1), f32),
            pltpu.VMEM((8, layers, width), f32),
            pltpu.VMEM((planes, layers, width), f32),
            pltpu.VMEM((layers, 8, 1, channels), f32),
            pltpu.VMEM((layers, planes, 1, channels), f32),
            pltpu.VMEM((8, 1, 128), f32),
            pltpu.VMEM((planes, 1, 128), f32),
            dma,
            dma((rows // BLOCK,)),
            dma((HALVES, 2, 5, n // 2)),
            dma((HALVES, 2, n)),
            dma((2 * layers, 2, 5, n // 2)),
            dma((2 * layers, 2, n)),
            dma((kinds, 8)),
            dma((kinds, 8)),
            dma((kinds, planes)),
            dma((kinds, planes)),
        ],
        compiler_params=pltpu.CompilerParams(
            collective_id=3, has_side_effects=True, vmem_limit_bytes=FULL_VMEM
        ),
        cost_estimate=pl.CostEstimate(
            flops=2 * rows * width * (width + 2 * layers * channels),
            bytes_accessed=4 * rows * width,
            transcendentals=0,
        ),
    )(lengths, hidden, joined, rotation)


def fits(n, hidden, rotation, cols):
    return (
        n % 8 == 0
        and cols % CHUNK == 0
        and rotation.shape[0] % CHUNK == 0
        and (8 * rotation.shape[0]) % 128 == 0
        and (8 * cols) % 128 == 0
        and hidden.shape[0] % BLOCK == 0
        and rotation.shape[1] % TILE == 0
        and rotation.shape[1] % (HALVES * ROT_TILE) == 0
        and hidden.shape[0] % (2 * STRIP) == 0
    )


def per_device(hidden, rotation, norm_gain, value_weight, output_weight, lengths):
    layers = norm_gain.shape[0]
    cols = value_weight.shape[2]
    own_len = lax.dynamic_slice_in_dim(lengths, lax.axis_index("dp"), 1)
    scaled = (norm_gain[:, :, None] * value_weight.astype(jnp.float32)).astype(jnp.bfloat16)
    width = rotation.shape[1]
    depth = value_weight.shape[1]
    joined = jnp.concatenate(
        [
            jnp.swapaxes(scaled, 1, 2).reshape(layers * cols, depth),
            output_weight.reshape(layers * cols, depth),
        ],
        axis=0,
    )
    n = lax.axis_size("dp")
    if fits(n, hidden, rotation, cols):
        out, loss = window(lengths, hidden, joined, rotation, layers)
        return (out, loss[0, 0])
    rotation_full = lax.all_gather(rotation, "dp", axis=0, tiled=True)
    value_q, rotated_o, tops = rotate_weights(
        joined, rotation_full, layers * cols, layers * cols, layers
    )
    tops = exchange(tops, n, 0)
    output_q = [
        fake_quant(
            rotated_o[l * cols : (l + 1) * cols], tops[l : l + 1] / 7.0 + EPS_SCALE
        ).astype(jnp.bfloat16)
        for l in range(layers)
    ]
    value_all = lax.all_gather(value_q, "dp", axis=0, tiled=False)
    output_all = []
    for l in range(layers):
        before = output_all[l - 1] if l > 0 else value_all
        local_o, _ = lax.optimization_barrier((output_q[l], before))
        output_all.append(lax.all_gather(local_o, "dp", axis=0, tiled=True))
    resid, act, msq, aerr = first_pass(hidden, rotation_full)
    loss = jnp.zeros((), jnp.float32)
    for l in range(layers):
        mixed, top = mix_pass(own_len, act, value_all, l, cols)
        vrange = exchange(top, n, 1)
        last = l == layers - 1
        res = update_pass(own_len, mixed, vrange, output_all[l], resid, msq, aerr, last)
        loss = loss + jnp.sum(res[0])
        if last:
            out = res[1]
        else:
            resid, act, msq, aerr = res[1:]
    count = jnp.sum(lengths).astype(jnp.float32)
    loss = exchange(jnp.full((1, 128), loss, jnp.float32), n, 2, total=True)[0, 0]
    return (out, loss / count)


def solution(mesh):
    return jax.shard_map(
        per_device,
        mesh=mesh,
        in_specs=(P("dp", None), P("dp", None), P(), P(None, None, "dp"), P(None, "dp", None), P()),
        out_specs=(P("dp", None), P()),
        check_vma=False,
    )
```

```python
import functools

import jax
import jax.numpy as jnp
from jax import lax
from jax.experimental import pallas as pl
from jax.experimental.pallas import tpu as pltpu
from jax.sharding import PartitionSpec as P

BLOCK = 256
CHUNK = 16
TILE = 512
VMEM_LIMIT = 60 * 1024 * 1024

EPS_NORM = 1e-06
EPS_SCALE = 1e-06
CLIP_RATIO = 0.9
POLY = (0.9999997571452157, -2.579687436847881, 2.6673586060553345, -1.5145036626283546, 0.48039577352173)


def soft_round(values):
    r = values - jnp.round(values)
    u = r * r
    p = jnp.float32(POLY[-1])
    for c in POLY[-2::-1]:
        p = p * u + jnp.float32(c)
    return values - p * (r - 4.0 * (r * u))


def fake_quant(values, step_size):
    inv = 1.0 / step_size
    return soft_round(jnp.clip(values * inv, -8.0, 7.0)) * step_size


def exchange_kernel(n, total, x_ref, out_ref, slots, send_sem, recv_sem):
    me = lax.axis_index("dp")
    barrier = pltpu.get_barrier_semaphore()

    def greet(k, _):
        pl.semaphore_signal(
            barrier,
            inc=1,
            device_id=(lax.rem(me + k, n),),
            device_id_type=pl.DeviceIdType.MESH,
        )
        return 0

    lax.fori_loop(1, n, greet, 0)
    pl.semaphore_wait(barrier, n - 1)

    def copy_to(peer, slot):
        return pltpu.make_async_remote_copy(
            src_ref=x_ref,
            dst_ref=slots.at[slot],
            send_sem=send_sem.at[peer],
            recv_sem=recv_sem.at[slot],
            device_id=(peer,),
            device_id_type=pl.DeviceIdType.MESH,
        )

    def push(k, _):
        copy_to(lax.rem(me + k, n), me).start()
        return 0

    lax.fori_loop(1, n, push, 0)
    slots[me] = x_ref[...]

    def settle(k, _):
        peer = lax.rem(me + k, n)
        copy = copy_to(peer, peer)
        copy.wait_send()
        copy.wait_recv()
        return 0

    lax.fori_loop(1, n, settle, 0)

    def fold(k, acc):
        return acc + slots[k] if total else jnp.maximum(acc, slots[k])

    out_ref[...] = lax.fori_loop(1, n, fold, slots[0])


def exchange(x, n, collective_id, total=False):
    return pl.pallas_call(
        functools.partial(exchange_kernel, n, total),
        name="exchange",
        in_specs=[pl.BlockSpec(memory_space=pltpu.VMEM)],
        out_specs=pl.BlockSpec(memory_space=pltpu.VMEM),
        out_shape=jax.ShapeDtypeStruct(x.shape, x.dtype),
        scratch_shapes=[
            pltpu.VMEM((n,) + x.shape, x.dtype),
            pltpu.SemaphoreType.DMA((n,)),
            pltpu.SemaphoreType.DMA((n,)),
        ],
        compiler_params=pltpu.CompilerParams(
            collective_id=collective_id, has_side_effects=True, vmem_limit_bytes=VMEM_LIMIT
        ),
        cost_estimate=pl.CostEstimate(flops=0, bytes_accessed=30_000_000, transcendentals=0),
    )(x)


def weight_kernel(v_rows, o_rows, layers, w_ref, r_ref, vq_ref, o_ref, top_ref, acc):
    j = pl.program_id(0)
    n = r_ref.shape[1]
    at = pl.ds(pl.multiple_of(j * n, n), n)
    prod = jnp.dot(w_ref[...], r_ref[...], preferred_element_type=jnp.float32)
    acc[:, at] = prod[:v_rows]
    o_ref[...] = prod[v_rows:]
    per = o_rows // layers
    for l in range(layers):
        lo = v_rows + l * per
        top_ref[l : l + 1, :] = jnp.max(jnp.abs(prod[lo : lo + per]), axis=0, keepdims=True)

    @pl.when(j == pl.num_programs(0) - 1)
    def _():
        def body(i, _):
            rows = pl.ds(pl.multiple_of(i * CHUNK, CHUNK), CHUNK)
            x = acc[rows, :]
            step = jnp.max(jnp.abs(x), axis=1, keepdims=True) / 7.0 + EPS_SCALE
            vq_ref[rows, :] = fake_quant(x, step).astype(jnp.bfloat16)
            return 0

        lax.fori_loop(0, v_rows // CHUNK, body, 0)


def rotate_weights(joined, rotation, v_rows, o_rows, layers):
    width = rotation.shape[1]
    depth = rotation.shape[0]
    return pl.pallas_call(
        functools.partial(weight_kernel, v_rows, o_rows, layers),
        name="rotate_weights",
        grid=(width // TILE,),
        in_specs=[
            pl.BlockSpec(joined.shape, lambda j: (0, 0)),
            pl.BlockSpec((depth, TILE), lambda j: (0, j)),
        ],
        out_specs=[
            pl.BlockSpec((v_rows, width), lambda j: (0, 0)),
            pl.BlockSpec((o_rows, TILE), lambda j: (0, j)),
            pl.BlockSpec((layers, TILE), lambda j: (0, j)),
        ],
        out_shape=[
            jax.ShapeDtypeStruct((v_rows, width), jnp.bfloat16),
            jax.ShapeDtypeStruct((o_rows, width), jnp.float32),
            jax.ShapeDtypeStruct((layers, width), jnp.float32),
        ],
        scratch_shapes=[pltpu.VMEM((v_rows, width), jnp.float32)],
        compiler_params=pltpu.CompilerParams(vmem_limit_bytes=VMEM_LIMIT),
        cost_estimate=pl.CostEstimate(
            flops=2 * joined.shape[0] * depth * width,
            bytes_accessed=2 * depth * width,
            transcendentals=0,
        ),
    )(joined, rotation)


def norm_rows(resid_ref, act_ref, msq_ref, aerr_ref):
    width = resid_ref.shape[1]

    def body(i, _):
        rows = pl.ds(pl.multiple_of(i * CHUNK, CHUNK), CHUNK)
        x = resid_ref[rows, :]
        mean_sq = jnp.sum(x * x, axis=1, keepdims=True) * (1.0 / width)
        inv = lax.rsqrt(mean_sq + EPS_NORM)
        step = CLIP_RATIO * (jnp.max(jnp.abs(x), axis=1, keepdims=True) * inv) / 7.0 + EPS_SCALE
        normed = x * inv
        act = fake_quant(normed, step)
        diff = act - normed
        act_ref[rows, :] = act.astype(jnp.bfloat16)
        msq_ref[rows, :] = mean_sq
        aerr_ref[rows, :] = jnp.sum(diff * diff, axis=1, keepdims=True)
        return 0

    lax.fori_loop(0, resid_ref.shape[0] // CHUNK, body, 0)


def first_kernel(h_ref, r_ref, resid_ref, act_ref, msq_ref, aerr_ref):
    def body(j, _):
        at = pl.ds(pl.multiple_of(j * TILE, TILE), TILE)
        resid_ref[:, at] = jnp.dot(h_ref[...], r_ref[:, at], preferred_element_type=jnp.float32)
        return 0

    lax.fori_loop(0, r_ref.shape[1] // TILE, body, 0)
    norm_rows(resid_ref, act_ref, msq_ref, aerr_ref)


def rows_spec(width):
    return pl.BlockSpec((BLOCK, width), lambda i, *_: (i, 0))


def whole_spec(shape):
    return pl.BlockSpec(shape, lambda i, *_: (0, 0), pipeline_mode=pl.Buffered(1))


def act_shapes(rows, width):
    return [
        jax.ShapeDtypeStruct((rows, width), jnp.float32),
        jax.ShapeDtypeStruct((rows, width), jnp.bfloat16),
        jax.ShapeDtypeStruct((rows, 1), jnp.float32),
        jax.ShapeDtypeStruct((rows, 1), jnp.float32),
    ]


def first_pass(hidden, rotation):
    rows, depth = hidden.shape
    width = rotation.shape[1]
    return pl.pallas_call(
        first_kernel,
        name="rotate_hidden",
        grid=(rows // BLOCK,),
        in_specs=[rows_spec(depth), whole_spec(rotation.shape)],
        out_specs=[rows_spec(width), rows_spec(width), rows_spec(1), rows_spec(1)],
        out_shape=act_shapes(rows, width),
        compiler_params=pltpu.CompilerParams(vmem_limit_bytes=VMEM_LIMIT),
        cost_estimate=pl.CostEstimate(
            flops=2 * rows * depth * width,
            bytes_accessed=2 * depth * width + 8 * rows * width,
            transcendentals=0,
        ),
    )(hidden, rotation)


def mix_kernel(len_ref, act_ref, v_ref, mixed_ref, top_ref):
    i = pl.program_id(0)
    tile = 256
    live = len_ref[0] - i * BLOCK
    mask = lax.broadcasted_iota(jnp.int32, (BLOCK, 1), 0) < live

    @pl.when(i == 0)
    def _():
        top_ref[...] = jnp.zeros_like(top_ref)

    cols = v_ref.shape[1]
    group = tile // cols

    def body(j, _):
        at = pl.ds(pl.multiple_of(j * tile, tile), tile)
        part = v_ref[pl.ds(j * group, group)]
        prod = lax.dot_general(
            act_ref[...],
            part.reshape(tile, part.shape[2]),
            (((1,), (1,)), ((), ())),
            preferred_element_type=jnp.float32,
        )
        mixed_ref[:, at] = prod
        peak = jnp.max(jnp.where(mask, jnp.abs(prod), 0.0), axis=0, keepdims=True)
        top_ref[:, at] = jnp.maximum(top_ref[:, at], peak)
        return 0

    lax.fori_loop(0, v_ref.shape[0] // group, body, 0)


def mix_pass(own_len, act, gathered, layer, cols):
    rows, width = act.shape
    n = gathered.shape[0]
    channels = n * cols
    if cols % 16 == 0:
        values = gathered
        spec = pl.BlockSpec(
            (n, cols, width), lambda i, *_: (0, layer, 0), pipeline_mode=pl.Buffered(1)
        )
    else:
        values = gathered[:, layer * cols : (layer + 1) * cols].reshape(-1, 128, width)
        spec = pl.BlockSpec(values.shape, lambda i, *_: (0, 0, 0), pipeline_mode=pl.Buffered(1))
    return pl.pallas_call(
        mix_kernel,
        name="mix",
        grid_spec=pltpu.PrefetchScalarGridSpec(
            num_scalar_prefetch=1,
            grid=(rows // BLOCK,),
            in_specs=[rows_spec(width), spec],
            out_specs=[
                rows_spec(channels),
                pl.BlockSpec((1, channels), lambda i, *_: (0, 0)),
            ],
        ),
        out_shape=[
            jax.ShapeDtypeStruct((rows, channels), jnp.float32),
            jax.ShapeDtypeStruct((1, channels), jnp.float32),
        ],
        compiler_params=pltpu.CompilerParams(vmem_limit_bytes=VMEM_LIMIT),
        cost_estimate=pl.CostEstimate(
            flops=2 * rows * channels * width,
            bytes_accessed=2 * channels * width + 4 * rows * width,
            transcendentals=0,
        ),
    )(own_len, act, values)


def update_kernel(last, len_ref, mixed_ref, vrange_ref, o_ref, resid_ref, msq_ref, aerr_ref, *rest):
    if last:
        loss_ref, out_ref, mix_buf = rest
    else:
        loss_ref, new_ref, act_ref, nmsq_ref, naerr_ref, mix_buf = rest
    live = len_ref[0] - pl.program_id(0) * BLOCK
    mask = lax.broadcasted_iota(jnp.int32, (BLOCK, 1), 0) < live
    step = CLIP_RATIO * vrange_ref[...] / 7.0 + EPS_SCALE

    def quant(i, _):
        rows = pl.ds(pl.multiple_of(i * CHUNK, CHUNK), CHUNK)
        x = mixed_ref[rows, :]
        mix = fake_quant(x, step)
        diff = mix - x
        mix_buf[rows, :] = mix.astype(jnp.bfloat16)
        loss_ref[rows, :] = jnp.sum(diff * diff, axis=1, keepdims=True)
        return 0

    lax.fori_loop(0, BLOCK // CHUNK, quant, 0)
    loss_ref[...] = jnp.where(mask, msq_ref[...] * (aerr_ref[...] + loss_ref[...]), 0.0)

    def body(j, _):
        at = pl.ds(pl.multiple_of(j * TILE, TILE), TILE)
        new = resid_ref[:, at] + jnp.dot(
            mix_buf[...], o_ref[:, at], preferred_element_type=jnp.float32
        )
        if last:
            out_ref[:, at] = jnp.where(mask, new, 0.0).astype(jnp.bfloat16)
        else:
            new_ref[:, at] = new
        return 0

    lax.fori_loop(0, o_ref.shape[1] // TILE, body, 0)
    if not last:
        norm_rows(new_ref, act_ref, nmsq_ref, naerr_ref)


def update_pass(own_len, mixed, vrange, outputs, resid, msq, aerr, last):
    rows, width = resid.shape
    channels = mixed.shape[1]
    out_specs = [rows_spec(1)]
    out_shape = [jax.ShapeDtypeStruct((rows, 1), jnp.float32)]
    if last:
        out_specs.append(rows_spec(width))
        out_shape.append(jax.ShapeDtypeStruct((rows, width), jnp.bfloat16))
    else:
        out_specs += [rows_spec(width), rows_spec(width), rows_spec(1), rows_spec(1)]
        out_shape += act_shapes(rows, width)
    return pl.pallas_call(
        functools.partial(update_kernel, last),
        name="update",
        grid_spec=pltpu.PrefetchScalarGridSpec(
            num_scalar_prefetch=1,
            grid=(rows // BLOCK,),
            in_specs=[
                rows_spec(channels),
                whole_spec((1, channels)),
                whole_spec(outputs.shape),
                rows_spec(width),
                rows_spec(1),
                rows_spec(1),
            ],
            out_specs=out_specs,
            scratch_shapes=[pltpu.VMEM((BLOCK, channels), jnp.bfloat16)],
        ),
        out_shape=out_shape,
        compiler_params=pltpu.CompilerParams(vmem_limit_bytes=VMEM_LIMIT),
        cost_estimate=pl.CostEstimate(
            flops=2 * rows * channels * width,
            bytes_accessed=2 * channels * width + 12 * rows * width,
            transcendentals=0,
        ),
    )(own_len, mixed, vrange, outputs, resid, msq, aerr)


MESH_ID = pl.DeviceIdType.MESH
FULL_VMEM = 67043328
STRIP = 128
ROT_TILE = 256
LANES = 128
HALVES = 2
CROSS_TENTHS = 2
ROT_STEP, ROT_GAP = 6.0, 12.0
STEP, GAP = 6.0, 17.0


class Place:
    def __init__(self, n):
        me = lax.axis_index("dp")
        core = lax.rem(me, 2)
        self.me, self.planes, self.core = me, n // 8, core
        self.z = me // 8
        self.stride2 = 2 + 2 * core
        self.stride3 = 4 - 2 * core
        self.bit2 = lax.rem(me // self.stride2, 2)
        self.bit3 = lax.rem(me // self.stride3, 2)
        self.to = [
            me + 8,
            me - 8,
            me + self.stride2 * (1 - 2 * self.bit2),
            me + self.stride3 * (1 - 2 * self.bit3),
            me + 1 - 2 * core,
        ]

    def origin(self, plane, flip2, flip3):
        bit2 = 1 - self.bit2 if flip2 else self.bit2
        bit3 = 1 - self.bit3 if flip3 else self.bit3
        return 8 * plane + self.core + self.stride2 * bit2 + self.stride3 * bit3

    def at_distance(self, s):
        if s == 0:
            return [(self.z, None)]
        return [(self.z - s, self.z >= s), (self.z + s, self.z + s < self.planes)]

    def on_planes(self, s, piece):
        if s == 0:
            piece(self.z)
            return

        def body(k, _):
            plane = self.z - s + 2 * s * k
            pl.when(jnp.logical_and(plane >= 0, plane < self.planes))(lambda: piece(plane))
            return 0

        lax.fori_loop(0, 2, body, 0)

    def greet(self):
        barrier = pltpu.get_barrier_semaphore()
        peers = [8 * self.z + lax.rem(self.me + k, 8) for k in range(1, 8)]
        peers += [lax.rem(self.me + 8 * k, 8 * self.planes) for k in range(1, self.planes)]
        for peer in peers:
            pl.semaphore_signal(barrier, inc=1, device_id=(peer,), device_id_type=MESH_ID)
        pl.semaphore_wait(barrier, len(peers))


def run_if(cond, fn):
    if cond is None:
        fn()
    else:
        pl.when(cond)(fn)


def start(copy):
    copy.start()


def sent(copy):
    copy.wait_send()


class Gather:
    def __init__(self, place, buf, send_sem, recv_sem, columns=slice(None)):
        self.place, self.buf, self.send_sem, self.recv_sem = place, buf, send_sem, recv_sem
        self.columns = columns

    def copy(self, o, d):
        return pltpu.make_async_remote_copy(
            src_ref=self.buf.at[o, :, self.columns],
            dst_ref=self.buf.at[o, :, self.columns],
            send_sem=self.send_sem.at[d, o // 2],
            recv_sem=self.recv_sem.at[o],
            device_id=(self.place.to[d],),
            device_id_type=MESH_ID,
        )

    def arrived(self, o):
        self.copy(o, 4).wait_recv()

    def up(self, o, act):
        pl.when(self.place.z < self.place.planes - 1)(lambda: act(self.copy(o, 0)))

    def down(self, o, act):
        pl.when(self.place.z > 0)(lambda: act(self.copy(o, 1)))

    def own(self, act=start):
        o = self.place.me
        self.up(o, act)
        self.down(o, act)
        for d in (2, 3, 4):
            act(self.copy(o, d))

    def line(self, s, act=start):
        for k, (plane, cond) in enumerate(self.place.at_distance(s)):

            def go(k=k, plane=plane):
                o = self.place.origin(plane, 0, 0)
                if act is start:
                    self.arrived(o)
                (self.up if k == 0 else self.down)(o, act)
                for d in (2, 3, 4):
                    act(self.copy(o, d))

            run_if(cond, go)

    def second(self, s, act=start):
        for plane, cond in self.place.at_distance(s):

            def go(plane=plane):
                o = self.place.origin(plane, 1, 0)
                if act is start:
                    self.arrived(o)
                for d in (3, 4):
                    act(self.copy(o, d))

            run_if(cond, go)

    def third(self, s, act=start):
        for plane, cond in self.place.at_distance(s):

            def go(plane=plane):
                for flip2 in (0, 1):
                    o = self.place.origin(plane, flip2, 1)
                    if act is start:
                        self.arrived(o)
                    act(self.copy(o, 4))

            run_if(cond, go)

    def other_core(self, s):
        for plane, cond in self.place.at_distance(s):

            def go(plane=plane):
                def body(q, _):
                    self.arrived(8 * plane + 2 * q + 1 - self.place.core)
                    return 0

                lax.fori_loop(0, 4, body, 0)

            run_if(cond, go)

    def events(self):
        planes = self.place.planes
        out = [(0, self.own, None)]
        for t in range(1, planes + 2):
            if t < planes:
                out.append((t, functools.partial(self.line, t), None))
            if t < planes + 1:
                out.append((t, functools.partial(self.second, t - 1), None))
            if t >= 2:
                out.append((t, functools.partial(self.third, t - 2), None))
                out.append((t + 0.3, functools.partial(self.other_core, t - 2), t - 2))
        return out

    def drain(self):
        self.own(sent)
        for s in range(self.place.planes):
            if s:
                self.line(s, sent)
            self.second(s, sent)
            self.third(s, sent)


class Cross(Gather):
    def second(self, act=start):
        o = self.place.origin(self.place.z, 1, 0)
        if act is start:
            self.arrived(o)
        self.up(o, act)
        self.down(o, act)
        for d in (3, 4):
            act(self.copy(o, d))

    def third(self, act=start):
        for flip2 in (0, 1):
            o = self.place.origin(self.place.z, flip2, 1)
            if act is start:
                self.arrived(o)
            self.up(o, act)
            self.down(o, act)
            act(self.copy(o, 4))

    def line(self, s, act=start):
        for k, (plane, cond) in enumerate(self.place.at_distance(s)):

            def go(k=k, plane=plane):
                def body(q, _):
                    o = 8 * plane + 2 * q + self.place.core
                    if act is start:
                        self.arrived(o)
                    (self.up if k == 0 else self.down)(o, act)
                    act(self.copy(o, 4))
                    return 0

                lax.fori_loop(0, 4, body, 0)

            run_if(cond, go)

    def events(self):
        out = [(0, self.own, None), (0.5, self.second, None), (1.2, self.third, None)]
        out.append((1.8, functools.partial(self.other_core, 0), 0))
        for s in range(1, self.place.planes):
            out.append((1.2 + s, functools.partial(self.line, s), None))
            out.append((2.3 + s, functools.partial(self.other_core, s), s))
        return out

    def drain(self):
        self.own(sent)
        self.second(sent)
        self.third(sent)
        for s in range(1, self.place.planes):
            self.line(s, sent)


class Exchange:
    def __init__(self, place, total, near, far, near_send, near_recv, far_send, far_recv):
        self.place, self.total, self.near, self.far = place, total, near, far
        self.sems = (near_send, near_recv, far_send, far_recv)
        self.spot = lax.rem(place.me, 8)

    def near_copy(self, k, slot):
        spot = lax.rem(self.spot + k, 8)
        return pltpu.make_async_remote_copy(
            src_ref=self.near.at[slot],
            dst_ref=self.near.at[slot],
            send_sem=self.sems[0].at[k],
            recv_sem=self.sems[1].at[slot],
            device_id=(8 * self.place.z + spot,),
            device_id_type=MESH_ID,
        )

    def far_copy(self, k, slot):
        plane = lax.rem(self.place.z + k, self.place.planes)
        return pltpu.make_async_remote_copy(
            src_ref=self.far.at[slot],
            dst_ref=self.far.at[slot],
            send_sem=self.sems[2].at[k],
            recv_sem=self.sems[3].at[slot],
            device_id=(8 * plane + self.spot,),
            device_id_type=MESH_ID,
        )

    def fold(self, slots, count):
        acc = slots[0]
        for k in range(1, count):
            acc = acc + slots[k] if self.total else jnp.maximum(acc, slots[k])
        return acc

    def begin(self, value):
        self.near[self.spot] = value
        for k in range(1, 8):
            self.near_copy(k, self.spot).start()

    def middle(self):
        for k in range(1, 8):
            self.near_copy(k, lax.rem(self.spot + k, 8)).wait_recv()
        self.far[self.place.z] = self.fold(self.near, 8)
        for k in range(1, self.place.planes):
            self.far_copy(k, self.place.z).start()

    def end(self):
        for k in range(1, self.place.planes):
            self.far_copy(k, lax.rem(self.place.z + k, self.place.planes)).wait_recv()
        return self.fold(self.far, self.place.planes)

    def drain(self):
        for k in range(1, 8):
            self.near_copy(k, self.spot).wait_send()
        for k in range(1, self.place.planes):
            self.far_copy(k, self.place.z).wait_send()


class Plan:
    def __init__(self):
        self.now, self.waits, self.work, self.count = 0.0, [], [], 0

    def wait(self, when, action):
        self.count += 1
        self.waits.append((when, self.count, action))

    def compute(self, rank, cost, action):
        self.count += 1
        self.work.append((rank, self.count, cost, action))

    def run(self):
        while self.waits or self.work:
            self.waits.sort(key=lambda w: w[:2])
            self.work.sort(key=lambda w: w[:2])
            if self.waits and (not self.work or self.waits[0][0] <= self.now):
                when, _, action = self.waits.pop(0)
                self.now = max(self.now, when)
                action()
            else:
                _, _, cost, action = self.work.pop(0)
                action()
                self.now += cost


def soft_parts(scaled):
    v = jnp.clip(scaled, -8.0, 7.0)
    r = v - jnp.round(v)
    u = r * r
    p = jnp.float32(POLY[-1])
    for c in POLY[-2::-1]:
        p = p * u + jnp.float32(c)
    return v - (p * (1.0 - 4.0 * u)) * r


def window_kernel(n, layers, *refs):
    len_ref, h_ref, gain_ref, v_ref, o_ref, r_ref, out_ref, loss_ref = refs[:8]
    (rbuf, vbuf, obuf, left, acc, act, mixed, mixq, top, msq, aerr, lossrow, size, scale) = refs[8:22]
    (ntops, ftops, ntop, ftop, nloss, floss) = refs[22:28]
    (local_sem, out_sem, rsend, rrecv, wsend, wrecv, xns, xnr, xfs, xfr) = refs[28:]
    place = Place(n)
    planes = place.planes
    rows, width = act.shape
    cols = vbuf.shape[2]
    vrows = layers * cols
    resid = acc.at[pl.ds(0, rows), :]
    wacc = acc.at[pl.ds(rows, 2 * vrows), :]
    channels = n * cols
    depth = 8 * r_ref.shape[0]
    lanes = 8 * cols
    half = width // HALVES
    live = len_ref[place.me]
    strips = rows // STRIP

    mine = pltpu.make_async_copy(r_ref, rbuf.at[place.me], local_sem.at[0])
    mine.start()
    loads = [pltpu.make_async_copy(h_ref, left.at[pl.ds(0, rows), :], local_sem.at[1])]
    for l in range(layers):
        to = left.at[pl.ds(rows + vrows + l * cols, cols), :]
        loads.append(pltpu.make_async_copy(o_ref.at[l], to, local_sem.at[2 + l]))
    for load in loads:
        load.start()
    place.greet()
    mine.wait()

    def both(buf, send_sem, recv_sem, lo, span):
        cut = span * CROSS_TENTHS // 10 // 128 * 128
        return (
            Gather(place, buf, send_sem.at[0], recv_sem.at[0], pl.ds(lo, span - cut)),
            Cross(place, buf, send_sem.at[1], recv_sem.at[1], pl.ds(lo + span - cut, cut)),
        )

    rots = [both(rbuf, rsend.at[q], rrecv.at[q], q * half, half) for q in range(HALVES)]
    gathers = []
    for l in range(layers):
        gathers.append(both(vbuf.at[l], wsend.at[2 * l], wrecv.at[2 * l], 0, width))
        gathers.append(both(obuf.at[l], wsend.at[2 * l + 1], wrecv.at[2 * l + 1], 0, width))

    def make(i, total, near, far):
        return Exchange(place, total, near, far, xns.at[i], xnr.at[i], xfs.at[i], xfr.at[i])

    tops = make(0, False, ntops, ftops)
    vranges = [make(1 + l, False, ntop.at[l], ftop.at[l]) for l in range(layers)]
    losses = make(1 + layers, True, nloss, floss)

    def prepare():
        for l in range(layers):
            scaled = gain_ref[l : l + 1, :] * v_ref[l].astype(jnp.float32)
            left[rows + l * cols : rows + (l + 1) * cols, :] = scaled.astype(jnp.bfloat16)
        for load in loads:
            load.wait()

    def product(q, first):
        def piece(plane):
            ks = pl.ds(pl.multiple_of(plane * depth, 128), depth)

            def body(j, _):
                at = pl.ds(pl.multiple_of(q * half + j * ROT_TILE, ROT_TILE), ROT_TILE)
                part = rbuf[pl.ds(8 * plane, 8), :, at].reshape(depth, ROT_TILE)
                prod = jnp.dot(left[:, ks], part, preferred_element_type=jnp.float32)
                if first:
                    acc[:, at] = prod
                else:
                    acc[:, at] += prod
                return 0

            lax.fori_loop(0, half // ROT_TILE, body, 0)

        return piece

    def quantize_values():
        for l in range(layers):
            for i in range(cols // CHUNK):
                x = wacc[l * cols + i * CHUNK : l * cols + (i + 1) * CHUNK, :]
                step = jnp.max(jnp.abs(x), axis=1, keepdims=True) / 7.0 + EPS_SCALE
                vbuf[l, place.me, i * CHUNK : (i + 1) * CHUNK, :] = fake_quant(x, step).astype(jnp.bfloat16)

    def begin_tops():
        peaks = [
            jnp.max(jnp.abs(wacc[vrows + l * cols : vrows + (l + 1) * cols, :]), axis=0, keepdims=True)
            for l in range(layers)
        ]
        tops.begin(jnp.concatenate(peaks, axis=0))

    def quantize_outputs():
        peaks = tops.end()
        for l in range(layers):
            lo = vrows + l * cols
            obuf[l, place.me] = fake_quant(
                wacc[lo : lo + cols, :], peaks[l : l + 1] / 7.0 + EPS_SCALE
            ).astype(jnp.bfloat16)

    def norm(p):
        at = pl.ds(pl.multiple_of(p * STRIP, STRIP), STRIP)
        total = jnp.zeros((STRIP, LANES), jnp.float32)
        peak = jnp.zeros((STRIP, LANES), jnp.float32)
        for j in range(width // LANES):
            x = resid[at, j * LANES : (j + 1) * LANES]
            total = total + x * x
            peak = jnp.maximum(peak, jnp.abs(x))
        mean_sq = jnp.sum(total, axis=1, keepdims=True) * (1.0 / width)
        inv = lax.rsqrt(mean_sq + EPS_NORM)
        step = CLIP_RATIO * (jnp.max(peak, axis=1, keepdims=True) * inv) / 7.0 + EPS_SCALE
        msq[at, :] = mean_sq
        size[at, :] = step
        scale[at, :] = inv / step
        wide_step = jnp.broadcast_to(size[at, :], (STRIP, LANES))
        wide_scale = jnp.broadcast_to(scale[at, :], (STRIP, LANES))
        err = jnp.zeros((STRIP, LANES), jnp.float32)
        for j in range(width // LANES):
            scaled = resid[at, j * LANES : (j + 1) * LANES] * wide_scale
            q = soft_parts(scaled)
            act[at, j * LANES : (j + 1) * LANES] = (q * wide_step).astype(jnp.bfloat16)
            diff = q - scaled
            err = err + diff * diff
        aerr[at, :] = jnp.sum(err, axis=1, keepdims=True) * (size[at, :] * size[at, :])

    def norm_strips(lo, hi):
        def body(p, _):
            norm(p)
            return 0

        lax.fori_loop(lo, hi, body, 0)

    def mix(l):
        def piece(plane):
            at = pl.ds(pl.multiple_of(plane * lanes, 128), lanes)
            part = vbuf[l, pl.ds(8 * plane, 8)].reshape(lanes, width)
            peak = jnp.zeros((1, lanes), jnp.float32)
            for b in range(rows // BLOCK):
                rs = slice(b * BLOCK, (b + 1) * BLOCK)
                prod = lax.dot_general(
                    act[rs, :], part, (((1,), (1,)), ((), ())), preferred_element_type=jnp.float32
                )
                mixed[rs, at] = prod
                mask = lax.broadcasted_iota(jnp.int32, (BLOCK, 1), 0) < live - b * BLOCK
                peak = jnp.maximum(
                    peak, jnp.max(jnp.where(mask, jnp.abs(prod), 0.0), axis=0, keepdims=True)
                )
            top[:, at] = peak

        return piece

    def quantize_mixed(l, lo, hi):
        def body(p, _):
            at = pl.ds(pl.multiple_of(p * STRIP, STRIP), STRIP)
            err = jnp.zeros((STRIP, LANES), jnp.float32)
            for j in range(channels // LANES):
                cut = slice(j * LANES, (j + 1) * LANES)
                step = CLIP_RATIO * top[:, cut] / 7.0 + EPS_SCALE
                inv = 1.0 / step
                x = mixed[at, cut]
                q = soft_parts(x * inv) * step
                mixq[at, cut] = q.astype(jnp.bfloat16)
                diff = q - x
                err = err + diff * diff
            mask = lax.broadcasted_iota(jnp.int32, (STRIP, 1), 0) < live - p * STRIP
            both = aerr[at, :] + jnp.sum(err, axis=1, keepdims=True)
            row = jnp.where(mask, msq[at, :] * both, 0.0)
            if l == 0:
                lossrow[at, :] = row
            else:
                lossrow[at, :] += row
            return 0

        lax.fori_loop(lo, hi, body, 0)

    def send_out(j):
        at = pl.ds(pl.multiple_of(j * TILE, TILE), TILE)
        return pltpu.make_async_copy(act.at[:, at], out_ref.at[:, at], out_sem.at[j])

    def update(l):
        def body(j, _):
            at = pl.ds(pl.multiple_of(j * TILE, TILE), TILE)
            part = obuf[l, :, :, at].reshape(channels, TILE)
            new = resid[:, at] + jnp.dot(mixq[...], part, preferred_element_type=jnp.float32)
            if l == layers - 1:
                mask = lax.broadcasted_iota(jnp.int32, (rows, 1), 0) < live
                act[:, at] = jnp.where(mask, new, 0.0).astype(jnp.bfloat16)
                send_out(j).start()
            else:
                resid[:, at] = new
            return 0

        lax.fori_loop(0, width // TILE, body, 0)

    plan = Plan()
    held = [[] for _ in gathers]
    open_ = [False] * len(gathers)

    def gather_waits(pair, base, step, arrived):
        here = [0] * planes
        for gather in pair[::-1]:
            for t, action, distance in gather.events():

                def go(action=action, distance=distance):
                    action()
                    if distance is not None:
                        here[distance] += 1
                        if here[distance] == len(pair):
                            arrived(distance)

                plan.wait(base + step * t, go)

    def rotated(q):
        def arrived(s):
            plan.compute(0, 2.5, lambda: (place.on_planes(s, product(q, s == 0)), rotation_done()))

        return arrived

    counts = {"rot": 0, "norm": [0] * layers, "mix": [0] * layers, "quant": [0] * layers, "out": [0] * layers}

    def rotation_done():
        counts["rot"] += 1
        if counts["rot"] < HALVES * planes:
            return
        quantize_values()
        base = plan.now
        gather_waits(gathers[0], base, STEP, shards(0))
        plan.wait(base + 0.1, begin_tops)
        plan.wait(base + 7.5, tops.middle)

        def outputs():
            quantize_outputs()
            for g in range(1, 2 * layers):
                gather_waits(gathers[g], max(plan.now, base + GAP * g), STEP, shards(g))

        plan.wait(base + 12.0, outputs)
        start_norm(0)

    def start_norm(l):
        for p in range(0, strips, 2):
            plan.compute(2, 3.0, lambda p=p: (norm_strips(p, p + 2), norm_done(l)))

    def norm_done(l):
        counts["norm"][l] += 2
        if counts["norm"][l] == strips:
            release(2 * l)

    def release(g):
        open_[g] = True
        for s in held[g]:
            add_piece(g, s)
        held[g] = []

    def shards(g):
        def arrived(s):
            if open_[g]:
                add_piece(g, s)
            else:
                held[g].append(s)

        return arrived

    def add_piece(g, s):
        l = g // 2
        if g % 2 == 0:
            plan.compute(3, 1.3, lambda: (place.on_planes(s, mix(l)), mix_done(l)))
            return
        counts["out"][l] += 1
        if counts["out"][l] == planes:
            plan.compute(5, 5.0, lambda: update_done(l))

    def mix_done(l):
        counts["mix"][l] += 1
        if counts["mix"][l] < planes:
            return
        vranges[l].begin(top[...])
        plan.wait(plan.now + 2.5, vranges[l].middle)

        def end():
            top[...] = vranges[l].end()
            for p in range(0, strips, 2):
                plan.compute(4, 1.2, lambda p=p: (quantize_mixed(l, p, p + 2), quant_done(l)))

        plan.wait(plan.now + 5.0, end)

    def quant_done(l):
        counts["quant"][l] += 2
        if counts["quant"][l] < strips:
            return
        if l == layers - 1:
            losses.begin(jnp.broadcast_to(jnp.sum(lossrow[...], axis=0, keepdims=True), (1, 128)))
            plan.wait(plan.now + 4.0, losses.middle)
        release(2 * l + 1)

    def update_done(l):
        update(l)
        if l < layers - 1:
            start_norm(l + 1)

    plan.wait(0.2, prepare)
    for q in range(HALVES):
        gather_waits(rots[q], q * ROT_GAP, ROT_STEP, rotated(q))
    plan.run()

    count = len_ref[0]
    for k in range(1, n):
        count = count + len_ref[k]
    loss_ref[...] = losses.end() / count.astype(jnp.float32)

    for pair in rots + gathers:
        for gather in pair:
            gather.drain()
    for exchanged in [tops, *vranges, losses]:
        exchanged.drain()
    for j in range(width // TILE):
        send_out(j).wait()


def window(lengths, hidden, norm_gain, value_weight, output_weight, rotation):
    n = lengths.shape[0]
    rows, width = hidden.shape
    layers, _, cols = value_weight.shape
    channels = n * cols
    stacked = rows + 2 * layers * cols
    planes = n // 8
    f32, bf16 = jnp.float32, jnp.bfloat16
    dma = pltpu.SemaphoreType.DMA
    kinds = 2 + layers
    vmem = pl.BlockSpec(memory_space=pltpu.VMEM)
    return pl.pallas_call(
        functools.partial(window_kernel, n, layers),
        name="window",
        in_specs=[
            pl.BlockSpec(memory_space=pltpu.SMEM),
            pl.BlockSpec(memory_space=pl.ANY),
            vmem,
            vmem,
            pl.BlockSpec(memory_space=pl.ANY),
            pl.BlockSpec(memory_space=pl.ANY),
        ],
        out_specs=[pl.BlockSpec(memory_space=pl.ANY), vmem],
        out_shape=[
            jax.ShapeDtypeStruct((rows, width), bf16),
            jax.ShapeDtypeStruct((1, 128), f32),
        ],
        scratch_shapes=[
            pltpu.VMEM((n,) + rotation.shape, bf16),
            pltpu.VMEM((layers, n, cols, width), bf16),
            pltpu.VMEM((layers, n, cols, width), bf16),
            pltpu.VMEM((stacked, width), bf16),
            pltpu.VMEM((stacked, width), f32),
            pltpu.VMEM((rows, width), bf16),
            pltpu.VMEM((rows, channels), f32),
            pltpu.VMEM((rows, channels), bf16),
            pltpu.VMEM((1, channels), f32),
            pltpu.VMEM((rows, 1), f32),
            pltpu.VMEM((rows, 1), f32),
            pltpu.VMEM((rows, 1), f32),
            pltpu.VMEM((rows, 1), f32),
            pltpu.VMEM((rows, 1), f32),
            pltpu.VMEM((8, layers, width), f32),
            pltpu.VMEM((planes, layers, width), f32),
            pltpu.VMEM((layers, 8, 1, channels), f32),
            pltpu.VMEM((layers, planes, 1, channels), f32),
            pltpu.VMEM((8, 1, 128), f32),
            pltpu.VMEM((planes, 1, 128), f32),
            dma((2 + layers,)),
            dma((width // TILE,)),
            dma((HALVES, 2, 5, n // 2)),
            dma((HALVES, 2, n)),
            dma((2 * layers, 2, 5, n // 2)),
            dma((2 * layers, 2, n)),
            dma((kinds, 8)),
            dma((kinds, 8)),
            dma((kinds, planes)),
            dma((kinds, planes)),
        ],
        compiler_params=pltpu.CompilerParams(
            collective_id=3, has_side_effects=True, vmem_limit_bytes=FULL_VMEM
        ),
        cost_estimate=pl.CostEstimate(
            flops=2 * rows * width * (width + 2 * layers * channels),
            bytes_accessed=4 * rows * width,
            transcendentals=0,
        ),
    )(lengths, hidden, norm_gain, jnp.swapaxes(value_weight, 1, 2), output_weight, rotation)


def fits(n, hidden, rotation, cols):
    return (
        n % 8 == 0
        and cols % CHUNK == 0
        and rotation.shape[0] % CHUNK == 0
        and (8 * rotation.shape[0]) % 128 == 0
        and (8 * cols) % 128 == 0
        and hidden.shape[0] % BLOCK == 0
        and rotation.shape[1] % TILE == 0
        and rotation.shape[1] % (HALVES * ROT_TILE) == 0
        and hidden.shape[0] % (2 * STRIP) == 0
    )


def per_device(hidden, rotation, norm_gain, value_weight, output_weight, lengths):
    layers = norm_gain.shape[0]
    cols = value_weight.shape[2]
    n = lax.axis_size("dp")
    if fits(n, hidden, rotation, cols):
        out, loss = window(lengths, hidden, norm_gain, value_weight, output_weight, rotation)
        return (out, loss[0, 0])
    own_len = lax.dynamic_slice_in_dim(lengths, lax.axis_index("dp"), 1)
    scaled = (norm_gain[:, :, None] * value_weight.astype(jnp.float32)).astype(jnp.bfloat16)
    width = rotation.shape[1]
    depth = value_weight.shape[1]
    joined = jnp.concatenate(
        [
            jnp.swapaxes(scaled, 1, 2).reshape(layers * cols, depth),
            output_weight.reshape(layers * cols, depth),
        ],
        axis=0,
    )
    rotation_full = lax.all_gather(rotation, "dp", axis=0, tiled=True)
    value_q, rotated_o, tops = rotate_weights(
        joined, rotation_full, layers * cols, layers * cols, layers
    )
    tops = exchange(tops, n, 0)
    output_q = [
        fake_quant(
            rotated_o[l * cols : (l + 1) * cols], tops[l : l + 1] / 7.0 + EPS_SCALE
        ).astype(jnp.bfloat16)
        for l in range(layers)
    ]
    value_all = lax.all_gather(value_q, "dp", axis=0, tiled=False)
    output_all = []
    for l in range(layers):
        before = output_all[l - 1] if l > 0 else value_all
        local_o, _ = lax.optimization_barrier((output_q[l], before))
        output_all.append(lax.all_gather(local_o, "dp", axis=0, tiled=True))
    resid, act, msq, aerr = first_pass(hidden, rotation_full)
    loss = jnp.zeros((), jnp.float32)
    for l in range(layers):
        mixed, top = mix_pass(own_len, act, value_all, l, cols)
        vrange = exchange(top, n, 1)
        last = l == layers - 1
        res = update_pass(own_len, mixed, vrange, output_all[l], resid, msq, aerr, last)
        loss = loss + jnp.sum(res[0])
        if last:
            out = res[1]
        else:
            resid, act, msq, aerr = res[1:]
    count = jnp.sum(lengths).astype(jnp.float32)
    loss = exchange(jnp.full((1, 128), loss, jnp.float32), n, 2, total=True)[0, 0]
    return (out, loss / count)


def solution(mesh):
    return jax.shard_map(
        per_device,
        mesh=mesh,
        in_specs=(P("dp", None), P("dp", None), P(), P(None, None, "dp"), P(None, "dp", None), P()),
        out_specs=(P("dp", None), P()),
        check_vma=False,
    )
```
